128 devices in a mesh: req: 2 (over core), seq: 64 (over x, z, y).
Axes of the slice: x: 4, y: 4, z: 4, core: 2. Of those that a mesh axis runs over, the one named last changes fastest.
Arguments:
- image_query: bfloat16 [1024, 1536], P(('req', 'seq')), parts along dimension 0, may hold values from -6 to 6
- image_key: bfloat16 [1024, 1536], P(('req', 'seq')), parts along dimension 0, may hold values from -6 to 6
- image_value: bfloat16 [1024, 1536], P(('req', 'seq')), parts along dimension 0, may hold values from -6 to 6
- text_query: bfloat16 [1024, 1536], P('req'), parts along dimension 0, may hold values from -6 to 6
- text_key: bfloat16 [1024, 1536], P('req'), parts along dimension 0, may hold values from -6 to 6
- text_value: bfloat16 [1024, 1536], P('req'), parts along dimension 0, may hold values from -6 to 6
- image_query_gain: float32 [128], replicated, may hold values from 1 to 8
- image_key_gain: float32 [128], replicated, may hold values from 1 to 8
- text_query_gain: float32 [128], replicated, may hold values from 1 to 2.5
- text_key_gain: float32 [128], replicated, may hold values from 1 to 2.5
- image_order: int32 [1024], P(('req', 'seq')), parts along dimension 0, may hold values from 0 to 511, each once
- text_length: int32 [2], P('req'), parts along dimension 0, may hold values from 256 to 512
Outputs:
- image_out: bfloat16 [1024, 1536], P(('req', 'seq')), parts along dimension 0
- text_out: bfloat16 [1024, 1536], P(('req', 'seq')), parts along dimension 0
The draws below stay inside these ranges and needn't reach their ends.
There are 2 independent parts, one for each index of `req`. The reference program is written for one: setup_inputs(seed, part) draws one part's arguments, and reference() takes and returns one part's arrays. A program takes and returns all parts, laid end to end along the dimension named above; an argument that names none is the same for every part. Nothing has to cross between parts.
Inputs may be any that keep to these rules, and one draw needn't show every extreme that they name: `image_order`: every position 0 to 511 appears once.
All inputs are finite; a program needn't handle non-finite values.
Results may differ from the reference program's by a relative error of at most 0.005.
The reference program's roundings to bfloat16 on the way (of `weights`) count: a program that leaves them out, or rounds other values in their place, can miss the bound.
Values may be sent and summed in bfloat16 or wider, within the bound.
No kernel may reach another device: no remote copies, remote signals or barrier semaphores. Data moves between devices by JAX's collectives and lax.ppermute only.
A program may use at most 64 MiB of HBM per device.

```python
import jax
import jax.numpy as jnp
from jax import lax

H = 12
HD = 128
TXT = 512
GRID_W = 64
TOK_DEV = 8
IMG = 512
N_SEQ = 64


def draw_image_query(key, part):
    queries = jax.random.normal(jax.random.fold_in(key, 1), (IMG, H * HD), jnp.float32)
    return jnp.clip(queries, -6.0, 6.0).astype(jnp.bfloat16)


def draw_image_key(key, part):
    keys_drawn = jax.random.normal(jax.random.fold_in(key, 2), (IMG, H * HD), jnp.float32)
    return jnp.clip(keys_drawn, -6.0, 6.0).astype(jnp.bfloat16)


def draw_image_query_gain(key, part):
    return jax.random.uniform(jax.random.fold_in(key, 5), (HD,), jnp.float32, 1.0, 2.5)


def draw_image_key_gain(key, part):
    return jax.random.uniform(jax.random.fold_in(key, 6), (HD,), jnp.float32, 1.0, 2.5)


def level_of(own_key, dims, cuts, low, top_value):
    level, own = 1.0, jax.random.fold_in(own_key, 6)
    for dim, parts in cuts:
        heights = jnp.exp(jax.random.uniform(jax.random.fold_in(own, dim), (parts,), jnp.float32, low / len(cuts), top_value / len(cuts)))
        level = level * jnp.repeat(heights, dims[dim] // parts).reshape([-1 if axis == dim else 1 for axis in range(len(dims))])
    return level


def bell_draw(stream_key, dims, deviation, limit, pieces=(), held_as=jnp.bfloat16):
    level = level_of(stream_key, dims, pieces, -0.22, 0.18) if pieces else 1.0
    values = jax.random.normal(stream_key, dims, jnp.float32) * deviation * level
    return jnp.minimum(jnp.maximum(values, -limit), limit).astype(held_as)


def setup_inputs(seed: int = 0, part: int = 0) -> dict:
    key_of = jax.random.split(jax.random.key(seed), 13)
    part_keys = jax.random.split(jax.random.fold_in(key_of[12], part), 13)
    image_query = draw_image_query(jax.random.fold_in(jax.random.fold_in(key_of[12], part), 71), part)
    image_key = draw_image_key(jax.random.fold_in(jax.random.fold_in(key_of[12], part), 71), part)
    image_value = bell_draw(part_keys[2], (IMG, H * HD), 1.0, 6.0, ((0, 64),))
    text_query = bell_draw(part_keys[3], (TXT, H * HD), 1.0, 6.0)
    text_key = bell_draw(part_keys[4], (TXT, H * HD), 1.0, 6.0)
    text_value = bell_draw(part_keys[5], (TXT, H * HD), 1.0, 6.0)
    image_query_gain = draw_image_query_gain(jax.random.fold_in(key_of[12], 71), part)
    image_key_gain = draw_image_key_gain(jax.random.fold_in(key_of[12], 71), part)
    text_query_gain = jnp.clip(jax.random.uniform(key_of[8], (HD,), jnp.float32, 1.0, 2.5), 1.0, 2.5)
    text_key_gain = jnp.clip(jax.random.uniform(key_of[9], (HD,), jnp.float32, 1.0, 2.5), 1.0, 2.5)
    image_order = jax.random.permutation(part_keys[10], IMG).astype(jnp.int32)
    text_length = jax.random.randint(part_keys[11], (1,), TXT // 2, TXT + 1).astype(jnp.int32)
    return {"image_query": image_query, "image_key": image_key, "image_value": image_value, "text_query": text_query, "text_key": text_key, "text_value": text_value, "image_query_gain": image_query_gain, "image_key_gain": image_key_gain, "text_query_gain": text_query_gain, "text_key_gain": text_key_gain, "image_order": image_order, "text_length": text_length}


epsilon = 1e-06
masked_score = -1e+30

def head_norm(values, norm_gain, head_count):
    row_count = values.shape[0]
    shaped = values.astype(jnp.float32).reshape(row_count, head_count, -1)
    mean_square = lax.optimization_barrier(jnp.mean(shaped * shaped, axis=-1, keepdims=True))
    return shaped * lax.rsqrt(mean_square + epsilon) * norm_gain

def rotate(normed, positions, half_length):
    row_count, head_count, head_dim = normed.shape
    pair_count = head_dim // 2
    pair_ids = jnp.arange(pair_count)
    first_axis = pair_ids < 8
    second = pair_ids < 36
    within = jnp.where(first_axis, pair_ids, jnp.where(second, pair_ids - 8, pair_ids - 36)).astype(jnp.float32)
    axis_dim = jnp.where(first_axis, 16.0, 56.0).astype(jnp.float32)
    frequency = jnp.power(jnp.float32(10000.0), -2.0 * within / axis_dim)
    image_index = positions // half_length
    inside = positions % half_length
    row_place = inside // GRID_W
    column_place = inside % GRID_W
    coordinate = jnp.where(first_axis[None, :], image_index[:, None], jnp.where(second[None, :], row_place[:, None], column_place[:, None])).astype(jnp.float32)
    angles = coordinate * frequency[None, :]
    cosine = jnp.cos(angles)[:, None, :]
    sine_part = jnp.sin(angles)[:, None, :]
    paired = normed.reshape(row_count, head_count, pair_count, 2)
    even_part = paired[..., 0]
    odd_part = paired[..., 1]
    turned = jnp.stack([even_part * cosine - odd_part * sine_part, even_part * sine_part + odd_part * cosine], axis=-1)
    return turned.reshape(row_count, head_count * head_dim)

def reference(image_query, image_key, image_value, text_query, text_key, text_value, image_query_gain, image_key_gain, text_query_gain, text_key_gain, image_order, text_length):
    head_count = image_query.shape[1] // HD
    half_length = IMG // 2
    query_img = lax.optimization_barrier(rotate(head_norm(image_query, image_query_gain, head_count), image_order, half_length).astype(jnp.bfloat16))
    key_img = lax.optimization_barrier(rotate(head_norm(image_key, image_key_gain, head_count), image_order, half_length).astype(jnp.bfloat16))
    query_txt = lax.optimization_barrier(head_norm(text_query, text_query_gain, head_count).reshape(TXT, -1).astype(jnp.bfloat16))
    key_txt = lax.optimization_barrier(head_norm(text_key, text_key_gain, head_count).reshape(TXT, -1).astype(jnp.bfloat16))
    all_keys = jnp.concatenate([key_txt, key_img], axis=0).astype(jnp.float32)
    all_values = jnp.concatenate([text_value, image_value], axis=0).astype(jnp.float32)
    key_count = all_keys.shape[0]
    key_heads = all_keys.reshape(key_count, head_count, HD)
    value_heads = all_values.reshape(key_count, head_count, HD)
    valid = jnp.concatenate([jnp.arange(TXT) < text_length[0], jnp.ones((IMG,), dtype=bool)])
    scaling = HD ** (-0.5)

    def attend(block):
        row_count = block.shape[0]
        query_heads = block.astype(jnp.float32).reshape(row_count, head_count, HD)
        scores = jnp.einsum('rhd,shd->rhs', query_heads, key_heads) * scaling
        scores = jnp.where(valid[None, None, :], scores, masked_score)
        row_max = lax.optimization_barrier(jnp.max(scores, axis=-1))
        expo = jnp.exp(scores - row_max[..., None])
        expo = jnp.where(valid[None, None, :], expo, 0.0)
        totals = lax.optimization_barrier(jnp.sum(expo, axis=-1))
        weights = lax.optimization_barrier(expo.astype(jnp.bfloat16)).astype(jnp.float32)
        blended = jnp.einsum('rhs,shd->rhd', weights, value_heads)
        return (blended / totals[..., None]).reshape(row_count, -1).astype(jnp.bfloat16)
    text_out = lax.map(attend, query_txt.reshape(N_SEQ, TXT // N_SEQ, -1)).reshape(TXT, -1)
    image_out = lax.map(attend, query_img.reshape(N_SEQ, TOK_DEV, -1)).reshape(IMG, -1)
    return (image_out, text_out)
```

```python
import math

import jax
import jax.numpy as jnp
from jax import lax
from jax.experimental import pallas as pl
from jax.experimental.pallas import tpu as pltpu
from jax.sharding import PartitionSpec as P

HD = 128
GRID_W = 64
SIDE = 4
EPS = 1e-06
MASKED = -1e30
SCALE = HD ** (-0.5)

VM = pl.BlockSpec(memory_space=pltpu.VMEM)
SM = pl.BlockSpec(memory_space=pltpu.SMEM)


def split_index(i):
    return i // (SIDE * SIDE), (i // SIDE) % SIDE, i % SIDE


def join_index(x, z, y):
    return ((x % SIDE) * SIDE + z % SIDE) * SIDE + y % SIDE


def shift(value, dx=0, dz=0, dy=0):
    pairs = []
    for i in range(SIDE**3):
        x, z, y = split_index(i)
        pairs.append((i, join_index(x + dx, z + dz, y + dy)))
    return lax.ppermute(value, "seq", pairs)


def head_norm(x, gain):
    mean_square = jnp.mean(x * x, axis=-1, keepdims=True)
    return x * lax.rsqrt(mean_square + EPS) * gain


def prep_kernel(heads, half, place, order, q_ref, k_ref, v_ref, qg, kg, o0, o1, o2, o3, q_s, k_s):
    rows = q_ref.shape[0]
    lane = lax.broadcasted_iota(jnp.int32, (rows, HD), 1)
    row = lax.broadcasted_iota(jnp.int32, (rows, HD), 0)
    pair = lane // 2
    first = pair < 8
    second = pair < 36
    within = jnp.where(first, pair, jnp.where(second, pair - 8, pair - 36)).astype(jnp.float32)
    dim = jnp.where(first, 16.0, 56.0)
    frequency = jnp.exp(within / dim * (-2.0 * math.log(10000.0)))
    t = jnp.zeros((rows, HD), jnp.int32)
    u = t
    w = t
    for i in range(rows):
        p = order[i]
        inside = p % half
        t = jnp.where(row == i, p // half, t)
        u = jnp.where(row == i, inside // GRID_W, u)
        w = jnp.where(row == i, inside % GRID_W, w)
    coordinate = jnp.where(first, t, jnp.where(second, u, w)).astype(jnp.float32)
    angle = coordinate * frequency
    cosine = jnp.cos(angle)
    sine = jnp.sin(angle)
    even = lane % 2 == 0
    sine = jnp.where(even, -sine, sine)
    for src, gain, dst in ((q_ref, qg, q_s), (k_ref, kg, k_s)):
        g = gain[...]
        for h in range(heads):
            x = head_norm(src[:, h * HD : (h + 1) * HD].astype(jnp.float32), g)
            partner = jnp.where(even, pltpu.roll(x, HD - 1, 1), pltpu.roll(x, 1, 1))
            dst[:, h * HD : (h + 1) * HD] = (x * cosine + partner * sine).astype(jnp.bfloat16)
    width = heads // SIDE * HD
    y = place[2]
    for d, out in enumerate((o0, o1, o2, o3)):
        start = pl.multiple_of(((y + d) % SIDE) * width, HD)
        out[:, 0:width] = k_s[:, pl.ds(start, width)]
        out[:, width : 2 * width] = v_ref[:, pl.ds(start, width)]
        out[:, 2 * width : 3 * width] = q_s[:, pl.ds(start, width)]


def pack_kernel(a0, a1, a2, a3, kv, q):
    rows = a0.shape[0]
    width = q.shape[1]
    for j, a in enumerate((a0, a1, a2, a3)):
        kv[j * rows : (j + 1) * rows, :] = a[:, : 2 * width]
        q[j * rows : (j + 1) * rows, :] = a[:, 2 * width :]


def text_kernel(place, q_ref, k_ref, v_ref, qg, kg, q_out, k_out, v_out):
    for src, gain, dst in ((q_ref, qg, q_out), (k_ref, kg, k_out)):
        g = gain[...]
        for h in range(src.shape[1] // HD):
            cols = slice(h * HD, (h + 1) * HD)
            dst[:, cols] = head_norm(src[:, cols].astype(jnp.float32), g).astype(jnp.bfloat16)
    v_out[...] = v_ref[...]


def attend_kernel(place, length, kv0, kv1, kv2, kv3, q0, q1, q2, q3, qt, kt, vt, out):
    kvs, qs = (kv0, kv1, kv2, kv3), (q0, q1, q2, q3)
    width = qt.shape[1]
    heads = width // HD
    text_keys = kt.shape[0]
    image_rows = SIDE * q0.shape[0]
    rows = image_rows + qt.shape[0]
    keys = text_keys + SIDE * kv0.shape[0]
    z, y = place[1], place[2]
    column = lax.broadcasted_iota(jnp.int32, (rows, keys), 1)
    valid = (column >= text_keys) | (column + z * text_keys < length[0])
    lane = lax.broadcasted_iota(jnp.int32, (rows, HD), 1)
    stats = jnp.zeros((rows, HD), jnp.float32)
    blended = []
    for h in range(heads):
        cols = slice(h * HD, (h + 1) * HD)
        vcols = slice(width + h * HD, width + (h + 1) * HD)
        query = jnp.concatenate([r[:, cols] for r in qs] + [qt[:, cols]], axis=0)
        key = jnp.concatenate([kt[:, cols]] + [r[:, cols] for r in kvs], axis=0)
        value = jnp.concatenate([vt[:, cols]] + [r[:, vcols] for r in kvs], axis=0)
        s = lax.dot_general(query, key, (((1,), (1,)), ((), ())), preferred_element_type=jnp.float32)
        s = jnp.where(valid, s * SCALE, MASKED)
        m = jnp.max(s, axis=1, keepdims=True).astype(jnp.bfloat16).astype(jnp.float32)
        e = jnp.exp(s - m)
        l = jnp.sum(e, axis=1, keepdims=True)
        blended.append(jnp.dot(e.astype(jnp.bfloat16), value, preferred_element_type=jnp.float32))
        low = l - l.astype(jnp.bfloat16).astype(jnp.float32)
        stats = jnp.where(lane == h, m, stats)
        stats = jnp.where(lane == 8 + h, l, stats)
        stats = jnp.where(lane == 16 + h, low, stats)
    blended.append(stats)
    for dz in range(SIDE):
        for dy in range(SIDE):
            i = dz * SIDE + dy
            there = ((z + SIDE - dz) % SIDE) * SIDE + (y + SIDE - dy) % SIDE
            for c, part in enumerate(blended):
                cols = slice(c * HD, (c + 1) * HD)
                out[there, 0:8, cols] = part[i * 8 : (i + 1) * 8].astype(jnp.bfloat16)
                begin = image_rows + i * 8
                out[i, 8:16, cols] = part[begin : begin + 8].astype(jnp.bfloat16)


def combine_kernel(got, image_out, text_out):
    heads = (got.shape[2] - HD) // HD
    width = heads * HD
    half = image_out.shape[0]
    for y in range(SIDE):
        stats = [got[z * SIDE + y, :, width:].astype(jnp.float32) for z in range(SIDE)]
        top = stats[0]
        for s in stats[1:]:
            top = jnp.maximum(top, s)
        factors = [jnp.exp(s - top) for s in stats]
        total = 0.0
        for s, f in zip(stats, factors):
            total = total + f * (pltpu.roll(s, HD - 8, 1) + pltpu.roll(s, HD - 16, 1))
        for h in range(heads):
            inverse = 1.0 / total[:, h : h + 1]
            acc = 0.0
            for z in range(SIDE):
                part = got[z * SIDE + y, :, h * HD : (h + 1) * HD].astype(jnp.float32)
                acc = acc + part * (factors[z][:, h : h + 1] * inverse)
            cols = slice(y * width + h * HD, y * width + (h + 1) * HD)
            image_out[:, cols] = acc[:half].astype(jnp.bfloat16)
            text_out[:, cols] = acc[half:].astype(jnp.bfloat16)


def local(
    image_query,
    image_key,
    image_value,
    text_query,
    text_key,
    text_value,
    image_query_gain,
    image_key_gain,
    text_query_gain,
    text_key_gain,
    image_order,
    text_length,
):
    rows, model = image_query.shape
    heads = model // HD
    width = model // SIDE
    text_rows = text_query.shape[0]
    block = text_rows // SIDE
    half = rows * SIDE**3 // 2
    x, z, y = split_index(lax.axis_index("seq"))
    place = jnp.stack([x, z, y]).astype(jnp.int32)
    bf = jnp.bfloat16
    struct = jax.ShapeDtypeStruct
    gains = [g.reshape(1, HD) for g in (image_query_gain, image_key_gain, text_query_gain, text_key_gain)]

    own = pl.pallas_call(
        lambda *refs: prep_kernel(heads, half, *refs),
        out_shape=[struct((rows, 3 * width), bf)] * SIDE,
        in_specs=[SM, SM] + [VM] * 5,
        out_specs=[VM] * SIDE,
        scratch_shapes=[pltpu.VMEM((rows, model), bf)] * 2,
        name="prep",
    )(place, image_order, image_query, image_key, image_value, gains[0], gains[1])

    from_y = [own[0]] + [shift(own[d], dy=d) for d in range(1, SIDE)]

    qt, kt, vt = pl.pallas_call(
        text_kernel,
        out_shape=[struct((block, width), bf)] * 3,
        grid_spec=pltpu.PrefetchScalarGridSpec(
            num_scalar_prefetch=1,
            grid=(1,),
            in_specs=[
                pl.BlockSpec((block, width), lambda i, p: (p[0], p[2])),
                pl.BlockSpec((block, width), lambda i, p: (p[1], p[2])),
                pl.BlockSpec((block, width), lambda i, p: (p[1], p[2])),
                pl.BlockSpec((1, HD), lambda i, p: (0, 0)),
                pl.BlockSpec((1, HD), lambda i, p: (0, 0)),
            ],
            out_specs=[pl.BlockSpec((block, width), lambda i, p: (0, 0))] * 3,
        ),
        cost_estimate=pl.CostEstimate(flops=20_000_000, bytes_accessed=600_000, transcendentals=0),
        name="text",
    )(place, text_query, text_key, text_value, gains[2], gains[3])

    kv, q = pl.pallas_call(
        pack_kernel,
        out_shape=[struct((SIDE * rows, 2 * width), bf), struct((SIDE * rows, width), bf)],
        in_specs=[VM] * SIDE,
        out_specs=[VM] * 2,
        name="pack",
    )(*from_y)

    kvs = [kv] + [shift(kv, dx=d) for d in range(1, SIDE)]
    qs = [q] + [shift(q, dz=d) for d in range(1, SIDE)]

    parts = SIDE * SIDE
    out_rows = rows + text_rows // SIDE**3
    partial = pl.pallas_call(
        attend_kernel,
        out_shape=struct((parts, out_rows, width + HD), bf),
        in_specs=[SM, SM] + [VM] * 11,
        out_specs=VM,
        name="attend",
    )(place, text_length, *kvs, *qs, qt, kt, vt)

    groups = [[x * parts + i for i in range(parts)] for x in range(SIDE)]
    got = lax.all_to_all(partial, "seq", 0, 0, axis_index_groups=groups, tiled=True)

    return pl.pallas_call(
        combine_kernel,
        out_shape=[struct((rows, model), bf), struct((out_rows - rows, model), bf)],
        in_specs=[VM],
        out_specs=[VM] * 2,
        name="combine",
    )(got)


def solution(mesh):
    token = P(("req", "seq"), None)
    text = P("req", None)
    return jax.shard_map(
        lambda *args: tuple(local(*args)),
        mesh=mesh,
        in_specs=(token, token, token, text, text, text, P(), P(), P(), P(), P(("req", "seq")), P("req")),
        out_specs=(token, token),
        check_vma=False,
    )
```

```python
import jax
import jax.numpy as jnp
import numpy as np
from jax import lax
from jax.experimental import pallas as pl
from jax.experimental.pallas import tpu as pltpu
from jax.sharding import PartitionSpec as P

HD = 128
GRID_W = 64
SIDE = 4
EPS = 1e-06
MASKED = -1e30
SCALE = HD ** (-0.5)

VM = pl.BlockSpec(memory_space=pltpu.VMEM)
SM = pl.BlockSpec(memory_space=pltpu.SMEM)
ANY = pl.BlockSpec(memory_space=pl.ANY)


def split_index(i):
    return i // (SIDE * SIDE), (i // SIDE) % SIDE, i % SIDE


def join_index(x, z, y):
    return ((x % SIDE) * SIDE + z % SIDE) * SIDE + y % SIDE


def shift(value, dx=0, dz=0, dy=0):
    pairs = []
    for i in range(SIDE**3):
        x, z, y = split_index(i)
        pairs.append((i, join_index(x + dx, z + dz, y + dy)))
    return in_vmem(lax.ppermute(value, "seq", pairs))


def in_vmem(value):
    return pltpu.with_memory_space_constraint(value, pltpu.VMEM)


def head_norm(x, gain):
    mean_square = jnp.mean(x * x, axis=-1, keepdims=True)
    return x * lax.rsqrt(mean_square + EPS) * gain


def frequencies():
    pair = np.arange(HD) // 2
    within = np.where(pair < 8, pair, np.where(pair < 36, pair - 8, pair - 36)).astype(np.float64)
    dim = np.where(pair < 8, 16.0, 56.0)
    return (10000.0 ** (-2.0 * within / dim)).astype(np.float32).reshape(1, HD)


def load(pairs, sems):
    copies = [pltpu.make_async_copy(src, dst, sems.at[i]) for i, (src, dst) in enumerate(pairs)]
    for c in copies:
        c.start()
    for c in copies:
        c.wait()


def prep_kernel(heads, half, order_h, freq_h, q_h, k_h, v_h, qg_h, kg_h, o0, o1, o2, o3, order, freq, q_in, k_in, v_in, qg, kg, q_s, k_s, sems):
    load(
        ((order_h, order), (freq_h, freq), (q_h, q_in), (k_h, k_in), (v_h, v_in), (qg_h, qg), (kg_h, kg)),
        sems,
    )
    rows = q_in.shape[0]
    lane = lax.broadcasted_iota(jnp.int32, (rows, HD), 1)
    row = lax.broadcasted_iota(jnp.int32, (rows, HD), 0)
    pair = lane // 2
    t = jnp.zeros((rows, HD), jnp.int32)
    u = t
    w = t
    for i in range(rows):
        p = order[i]
        inside = p % half
        t = jnp.where(row == i, p // half, t)
        u = jnp.where(row == i, inside // GRID_W, u)
        w = jnp.where(row == i, inside % GRID_W, w)
    coordinate = jnp.where(pair < 8, t, jnp.where(pair < 36, u, w)).astype(jnp.float32)
    angle = coordinate * freq[...]
    cosine = jnp.cos(angle)
    sine = jnp.sin(angle)
    even = lane % 2 == 0
    sine = jnp.where(even, -sine, sine)
    for src, gain, dst in ((q_in, qg, q_s), (k_in, kg, k_s)):
        g = gain[...]
        for h in range(heads):
            x = head_norm(src[:, h * HD : (h + 1) * HD].astype(jnp.float32), g)
            partner = jnp.where(even, pltpu.roll(x, HD - 1, 1), pltpu.roll(x, 1, 1))
            dst[:, h * HD : (h + 1) * HD] = (x * cosine + partner * sine).astype(jnp.bfloat16)
    width = heads // SIDE * HD
    y = lax.axis_index("seq") % SIDE
    for d, out in enumerate((o0, o1, o2, o3)):
        start = pl.multiple_of(((y + d) % SIDE) * width, HD)
        out[:, 0:width] = k_s[:, pl.ds(start, width)]
        out[:, width : 2 * width] = v_in[:, pl.ds(start, width)]
        out[:, 2 * width : 3 * width] = q_s[:, pl.ds(start, width)]


def pack_kernel(a0, a1, a2, a3, order_only, kv, q):
    rows = a0.shape[0]
    width = q.shape[1]
    for j, a in enumerate((a0, a1, a2, a3)):
        kv[j * rows : (j + 1) * rows, :] = a[:, : 2 * width]
        q[j * rows : (j + 1) * rows, :] = a[:, 2 * width :]


def text_kernel(q_h, k_h, v_h, qg_h, kg_h, length_h, q_out, k_out, v_out, bias, length, q_in, k_in, qg, kg, sems):
    block, width = q_in.shape
    x, z, y = split_index(lax.axis_index("seq"))
    cols = pl.ds(pl.multiple_of(y * width, HD), width)
    q_rows = pl.ds(pl.multiple_of(x * block, block), block)
    k_rows = pl.ds(pl.multiple_of(z * block, block), block)
    load(
        (
            (length_h, length),
            (q_h.at[q_rows, cols], q_in),
            (k_h.at[k_rows, cols], k_in),
            (v_h.at[k_rows, cols], v_out),
            (qg_h, qg),
            (kg_h, kg),
        ),
        sems,
    )
    for src, gain, dst in ((q_in, qg, q_out), (k_in, kg, k_out)):
        g = gain[...]
        for h in range(width // HD):
            at = slice(h * HD, (h + 1) * HD)
            dst[:, at] = head_norm(src[:, at].astype(jnp.float32), g).astype(jnp.bfloat16)
    key = lax.broadcasted_iota(jnp.int32, bias.shape, 1) + z * block
    bias[...] = jnp.where(key < length[0], 0.0, MASKED)


def attend_kernel(kv0, kv1, kv2, kv3, q0, q1, q2, q3, qt, kt, vt, bias, out):
    kvs, qs = (kv0, kv1, kv2, kv3), (q0, q1, q2, q3)
    width = qt.shape[1]
    heads = width // HD
    text_keys = kt.shape[0]
    image_rows = SIDE * q0.shape[0]
    rows = image_rows + qt.shape[0]
    _, z, y = split_index(lax.axis_index("seq"))
    masked = bias[0:1, :]
    lane = lax.broadcasted_iota(jnp.int32, (rows, HD), 1)
    stats = jnp.zeros((rows, HD), jnp.float32)
    blended = []
    for h in range(heads):
        cols = slice(h * HD, (h + 1) * HD)
        vcols = slice(width + h * HD, width + (h + 1) * HD)
        query = jnp.concatenate([r[:, cols] for r in qs] + [qt[:, cols]], axis=0)
        key = jnp.concatenate([kt[:, cols]] + [r[:, cols] for r in kvs], axis=0)
        value = jnp.concatenate([vt[:, cols]] + [r[:, vcols] for r in kvs], axis=0)
        s = lax.dot_general(query, key, (((1,), (1,)), ((), ())), preferred_element_type=jnp.float32)
        s = jnp.concatenate([s[:, :text_keys] * SCALE + masked, s[:, text_keys:] * SCALE], axis=1)
        m = jnp.max(s, axis=1, keepdims=True)
        e = jnp.exp(s - m)
        l = jnp.sum(e, axis=1, keepdims=True)
        blended.append(jnp.dot(e.astype(jnp.bfloat16), value, preferred_element_type=jnp.float32))
        for first, value in ((h, m), (24 + h, l)):
            for piece in range(3 if first == h else 2):
                stats = jnp.where(lane == first + 8 * piece, value, stats)
                value = value - value.astype(jnp.bfloat16).astype(jnp.float32)
    blended.append(stats)
    for dz in range(SIDE):
        for dy in range(SIDE):
            i = dz * SIDE + dy
            there = ((z + SIDE - dz) % SIDE) * SIDE + (y + SIDE - dy) % SIDE
            for c, part in enumerate(blended):
                cols = slice(c * HD, (c + 1) * HD)
                out[there, 0:8, cols] = part[i * 8 : (i + 1) * 8].astype(jnp.bfloat16)
                begin = image_rows + i * 8
                out[i, 8:16, cols] = part[begin : begin + 8].astype(jnp.bfloat16)


def combine_kernel(got, image_out, text_out):
    heads = (got.shape[2] - HD) // HD
    width = heads * HD
    half = image_out.shape[0]
    for y in range(SIDE):
        stats = [got[z * SIDE + y, :, width:].astype(jnp.float32) for z in range(SIDE)]
        peaks = [s + pltpu.roll(s, HD - 8, 1) + pltpu.roll(s, HD - 16, 1) for s in stats]
        sums = [pltpu.roll(s, HD - 24, 1) + pltpu.roll(s, HD - 32, 1) for s in stats]
        top = peaks[0]
        for p in peaks[1:]:
            top = jnp.maximum(top, p)
        factors = [jnp.exp(p - top) for p in peaks]
        total = 0.0
        for s, f in zip(sums, factors):
            total = total + f * s
        for h in range(heads):
            inverse = 1.0 / total[:, h : h + 1]
            acc = 0.0
            for z in range(SIDE):
                part = got[z * SIDE + y, :, h * HD : (h + 1) * HD].astype(jnp.float32)
                acc = acc + part * (factors[z][:, h : h + 1] * inverse)
            cols = slice(y * width + h * HD, y * width + (h + 1) * HD)
            image_out[:, cols] = acc[:half].astype(jnp.bfloat16)
            text_out[:, cols] = acc[half:].astype(jnp.bfloat16)


def local(
    image_query,
    image_key,
    image_value,
    text_query,
    text_key,
    text_value,
    image_query_gain,
    image_key_gain,
    text_query_gain,
    text_key_gain,
    image_order,
    text_length,
):
    rows, model = image_query.shape
    heads = model // HD
    width = model // SIDE
    text_rows = text_query.shape[0]
    block = text_rows // SIDE
    half = rows * SIDE**3 // 2
    bf, f32 = jnp.bfloat16, jnp.float32
    struct = jax.ShapeDtypeStruct
    gains = [g.reshape(1, HD) for g in (image_query_gain, image_key_gain, text_query_gain, text_key_gain)]

    own = pl.pallas_call(
        lambda *refs: prep_kernel(heads, half, *refs),
        out_shape=[pltpu.VMEM((rows, 3 * width), bf)] * SIDE,
        in_specs=[ANY] * 7,
        out_specs=[VM] * SIDE,
        scratch_shapes=[
            pltpu.SMEM((rows,), jnp.int32),
            pltpu.VMEM((1, HD), f32),
            pltpu.VMEM((rows, model), bf),
            pltpu.VMEM((rows, model), bf),
            pltpu.VMEM((rows, model), bf),
            pltpu.VMEM((1, HD), f32),
            pltpu.VMEM((1, HD), f32),
            pltpu.VMEM((rows, model), bf),
            pltpu.VMEM((rows, model), bf),
            pltpu.SemaphoreType.DMA((7,)),
        ],
        name="prep",
    )(image_order, jnp.asarray(frequencies()), image_query, image_key, image_value, gains[0], gains[1])

    from_y = [own[0]] + [shift(own[d], dy=d) for d in range(1, SIDE)]

    qt, kt, vt, bias = pl.pallas_call(
        text_kernel,
        out_shape=[pltpu.VMEM((block, width), bf)] * 3 + [pltpu.VMEM((8, block), f32)],
        in_specs=[ANY] * 6,
        out_specs=[VM] * 4,
        scratch_shapes=[
            pltpu.SMEM((1,), jnp.int32),
            pltpu.VMEM((block, width), bf),
            pltpu.VMEM((block, width), bf),
            pltpu.VMEM((1, HD), f32),
            pltpu.VMEM((1, HD), f32),
            pltpu.SemaphoreType.DMA((6,)),
        ],
        cost_estimate=pl.CostEstimate(flops=20_000_000, bytes_accessed=600_000, transcendentals=0),
        name="text",
    )(text_query, text_key, text_value, gains[2], gains[3], text_length)

    kv, q = pl.pallas_call(
        pack_kernel,
        out_shape=[pltpu.VMEM((SIDE * rows, 2 * width), bf), pltpu.VMEM((SIDE * rows, width), bf)],
        in_specs=[VM] * SIDE + [VM],
        out_specs=[VM] * 2,
        name="pack",
    )(*from_y, bias)

    kvs = [kv] + [shift(kv, dx=d) for d in range(1, SIDE)]
    qs = [q] + [shift(q, dz=d) for d in range(1, SIDE)]

    parts = SIDE * SIDE
    out_rows = rows + text_rows // SIDE**3
    partial = pl.pallas_call(
        attend_kernel,
        out_shape=pltpu.VMEM((parts, out_rows, width + HD), bf),
        in_specs=[VM] * 12,
        out_specs=VM,
        name="attend",
    )(*kvs, *qs, qt, kt, vt, bias)

    groups = [[x * parts + i for i in range(parts)] for x in range(SIDE)]
    got = in_vmem(lax.all_to_all(partial, "seq", 0, 0, axis_index_groups=groups, tiled=True))

    return pl.pallas_call(
        combine_kernel,
        out_shape=[struct((rows, model), bf), struct((out_rows - rows, model), bf)],
        in_specs=[VM],
        out_specs=[VM] * 2,
        name="combine",
    )(got)


def solution(mesh):
    token = P(("req", "seq"), None)
    text = P("req", None)
    return jax.shard_map(
        lambda *args: tuple(local(*args)),
        mesh=mesh,
        in_specs=(token, token, token, text, text, text, P(), P(), P(), P(), P(("req", "seq")), P("req")),
        out_specs=(token, token),
        check_vma=False,
    )
```

```python
import jax
import jax.numpy as jnp
import numpy as np
from jax import lax
from jax.experimental import pallas as pl
from jax.experimental.pallas import tpu as pltpu
from jax.sharding import PartitionSpec as P

HD = 128
GRID_W = 64
SIDE = 4
EPS = 1e-06
MASKED = -1e30
SCALE = HD ** (-0.5)

VM = pl.BlockSpec(memory_space=pltpu.VMEM)
SM = pl.BlockSpec(memory_space=pltpu.SMEM)
HB = pl.BlockSpec(memory_space=pltpu.HBM)


def split_index(i):
    return i // (SIDE * SIDE), (i // SIDE) % SIDE, i % SIDE


def join_index(x, z, y):
    return ((x % SIDE) * SIDE + z % SIDE) * SIDE + y % SIDE


def shift(value, dx=0, dz=0, dy=0):
    pairs = []
    for i in range(SIDE**3):
        x, z, y = split_index(i)
        pairs.append((i, join_index(x + dx, z + dz, y + dy)))
    return in_vmem(lax.ppermute(value, "seq", pairs))


def in_vmem(value):
    return pltpu.with_memory_space_constraint(value, pltpu.VMEM)


def vmem_call(kernel, **options):
    call = pl.pallas_call(kernel, **options)
    return lambda *args: jax.tree.map(in_vmem, call(*args))


def head_norm(x, gain):
    mean_square = jnp.mean(x * x, axis=-1, keepdims=True)
    return x * lax.rsqrt(mean_square + EPS) * gain


def frequencies():
    pair = np.arange(HD) // 2
    within = np.where(pair < 8, pair, np.where(pair < 36, pair - 8, pair - 36)).astype(np.float64)
    dim = np.where(pair < 8, 16.0, 56.0)
    return (10000.0 ** (-2.0 * within / dim)).astype(np.float32).reshape(1, HD)


def load(pairs, sems):
    copies = [pltpu.make_async_copy(src, dst, sems.at[i]) for i, (src, dst) in enumerate(pairs)]
    for c in copies:
        c.start()
    for c in copies:
        c.wait()


def prep_kernel(heads, half, order_h, freq_h, q_h, k_h, v_h, qg_h, kg_h, o0, o1, o2, o3, order, freq, q_in, k_in, v_in, qg, kg, q_s, k_s, sems):
    load(
        ((order_h, order), (freq_h, freq), (q_h, q_in), (k_h, k_in), (v_h, v_in), (qg_h, qg), (kg_h, kg)),
        sems,
    )
    rows = q_in.shape[0]
    lane = lax.broadcasted_iota(jnp.int32, (rows, HD), 1)
    row = lax.broadcasted_iota(jnp.int32, (rows, HD), 0)
    pair = lane // 2
    t = jnp.zeros((rows, HD), jnp.int32)
    u = t
    w = t
    for i in range(rows):
        p = order[i]
        inside = p % half
        t = jnp.where(row == i, p // half, t)
        u = jnp.where(row == i, inside // GRID_W, u)
        w = jnp.where(row == i, inside % GRID_W, w)
    coordinate = jnp.where(pair < 8, t, jnp.where(pair < 36, u, w)).astype(jnp.float32)
    angle = coordinate * freq[...]
    cosine = jnp.cos(angle)
    sine = jnp.sin(angle)
    even = lane % 2 == 0
    sine = jnp.where(even, -sine, sine)
    for src, gain, dst in ((q_in, qg, q_s), (k_in, kg, k_s)):
        g = gain[...]
        for h in range(heads):
            x = head_norm(src[:, h * HD : (h + 1) * HD].astype(jnp.float32), g)
            partner = jnp.where(even, pltpu.roll(x, HD - 1, 1), pltpu.roll(x, 1, 1))
            dst[:, h * HD : (h + 1) * HD] = (x * cosine + partner * sine).astype(jnp.bfloat16)
    width = heads // SIDE * HD
    y = lax.axis_index("seq") % SIDE
    for d, out in enumerate((o0, o1, o2, o3)):
        start = pl.multiple_of(((y + d) % SIDE) * width, HD)
        out[:, 0:width] = k_s[:, pl.ds(start, width)]
        out[:, width : 2 * width] = v_in[:, pl.ds(start, width)]
        out[:, 2 * width : 3 * width] = q_s[:, pl.ds(start, width)]


def pack_kernel(a0, a1, a2, a3, order_only, kv, q):
    rows = a0.shape[0]
    width = q.shape[1]
    for j, a in enumerate((a0, a1, a2, a3)):
        kv[j * rows : (j + 1) * rows, :] = a[:, : 2 * width]
        q[j * rows : (j + 1) * rows, :] = a[:, 2 * width :]


def text_kernel(q_h, k_h, v_h, qg_h, kg_h, length_h, q_out, k_out, v_out, bias, length, q_in, k_in, qg, kg, sems):
    block, width = q_in.shape
    x, z, y = split_index(lax.axis_index("seq"))
    cols = pl.ds(pl.multiple_of(y * width, HD), width)
    q_rows = pl.ds(pl.multiple_of(x * block, block), block)
    k_rows = pl.ds(pl.multiple_of(z * block, block), block)
    load(
        (
            (length_h, length),
            (q_h.at[q_rows, cols], q_in),
            (k_h.at[k_rows, cols], k_in),
            (v_h.at[k_rows, cols], v_out),
            (qg_h, qg),
            (kg_h, kg),
        ),
        sems,
    )
    for src, gain, dst in ((q_in, qg, q_out), (k_in, kg, k_out)):
        g = gain[...]
        for h in range(width // HD):
            at = slice(h * HD, (h + 1) * HD)
            dst[:, at] = head_norm(src[:, at].astype(jnp.float32), g).astype(jnp.bfloat16)
    key = lax.broadcasted_iota(jnp.int32, bias.shape, 1) + z * block
    bias[...] = jnp.where(key < length[0], 0.0, MASKED)


def attend_kernel(kv0, kv1, kv2, kv3, q0, q1, q2, q3, qt, kt, vt, bias, out):
    kvs, qs = (kv0, kv1, kv2, kv3), (q0, q1, q2, q3)
    width = qt.shape[1]
    heads = width // HD
    text_keys = kt.shape[0]
    image_rows = SIDE * q0.shape[0]
    rows = image_rows + qt.shape[0]
    _, z, y = split_index(lax.axis_index("seq"))
    masked = bias[0:1, :]
    lane = lax.broadcasted_iota(jnp.int32, (rows, HD), 1)
    stats = jnp.zeros((rows, HD), jnp.float32)
    blended = []
    for h in range(heads):
        cols = slice(h * HD, (h + 1) * HD)
        vcols = slice(width + h * HD, width + (h + 1) * HD)
        query = jnp.concatenate([r[:, cols] for r in qs] + [qt[:, cols]], axis=0)
        key = jnp.concatenate([kt[:, cols]] + [r[:, cols] for r in kvs], axis=0)
        value = jnp.concatenate([vt[:, cols]] + [r[:, vcols] for r in kvs], axis=0)
        s = lax.dot_general(query, key, (((1,), (1,)), ((), ())), preferred_element_type=jnp.float32)
        s = jnp.concatenate([s[:, :text_keys] * SCALE + masked, s[:, text_keys:] * SCALE], axis=1)
        m = jnp.max(s, axis=1, keepdims=True)
        e = jnp.exp(s - m)
        l = jnp.sum(e, axis=1, keepdims=True)
        blended.append(jnp.dot(e.astype(jnp.bfloat16), value, preferred_element_type=jnp.float32))
        for first, value in ((h, m), (24 + h, l)):
            for piece in range(3 if first == h else 2):
                stats = jnp.where(lane == first + 8 * piece, value, stats)
                value = value - value.astype(jnp.bfloat16).astype(jnp.float32)
    blended.append(stats)
    for dz in range(SIDE):
        for dy in range(SIDE):
            i = dz * SIDE + dy
            there = ((z + SIDE - dz) % SIDE) * SIDE + (y + SIDE - dy) % SIDE
            for c, part in enumerate(blended):
                cols = slice(c * HD, (c + 1) * HD)
                out[there, 0:8, cols] = part[i * 8 : (i + 1) * 8].astype(jnp.bfloat16)
                begin = image_rows + i * 8
                out[i, 8:16, cols] = part[begin : begin + 8].astype(jnp.bfloat16)


def combine_kernel(got, image_out, text_out):
    heads = (got.shape[2] - HD) // HD
    width = heads * HD
    half = image_out.shape[0]
    for y in range(SIDE):
        stats = [got[z * SIDE + y, :, width:].astype(jnp.float32) for z in range(SIDE)]
        peaks = [s + pltpu.roll(s, HD - 8, 1) + pltpu.roll(s, HD - 16, 1) for s in stats]
        sums = [pltpu.roll(s, HD - 24, 1) + pltpu.roll(s, HD - 32, 1) for s in stats]
        top = peaks[0]
        for p in peaks[1:]:
            top = jnp.maximum(top, p)
        factors = [jnp.exp(p - top) for p in peaks]
        total = 0.0
        for s, f in zip(sums, factors):
            total = total + f * s
        for h in range(heads):
            inverse = 1.0 / total[:, h : h + 1]
            acc = 0.0
            for z in range(SIDE):
                part = got[z * SIDE + y, :, h * HD : (h + 1) * HD].astype(jnp.float32)
                acc = acc + part * (factors[z][:, h : h + 1] * inverse)
            cols = slice(y * width + h * HD, y * width + (h + 1) * HD)
            image_out[:, cols] = acc[:half].astype(jnp.bfloat16)
            text_out[:, cols] = acc[half:].astype(jnp.bfloat16)


def local(
    image_query,
    image_key,
    image_value,
    text_query,
    text_key,
    text_value,
    image_query_gain,
    image_key_gain,
    text_query_gain,
    text_key_gain,
    image_order,
    text_length,
):
    rows, model = image_query.shape
    heads = model // HD
    width = model // SIDE
    text_rows = text_query.shape[0]
    block = text_rows // SIDE
    half = rows * SIDE**3 // 2
    bf, f32 = jnp.bfloat16, jnp.float32
    struct = jax.ShapeDtypeStruct
    gains = [g.reshape(1, HD) for g in (image_query_gain, image_key_gain, text_query_gain, text_key_gain)]

    own = vmem_call(
        lambda *refs: prep_kernel(heads, half, *refs),
        out_shape=[pltpu.VMEM((rows, 3 * width), bf)] * SIDE,
        in_specs=[HB] * 7,
        out_specs=[VM] * SIDE,
        scratch_shapes=[
            pltpu.SMEM((rows,), jnp.int32),
            pltpu.VMEM((1, HD), f32),
            pltpu.VMEM((rows, model), bf),
            pltpu.VMEM((rows, model), bf),
            pltpu.VMEM((rows, model), bf),
            pltpu.VMEM((1, HD), f32),
            pltpu.VMEM((1, HD), f32),
            pltpu.VMEM((rows, model), bf),
            pltpu.VMEM((rows, model), bf),
            pltpu.SemaphoreType.DMA((7,)),
        ],
        name="prep",
    )(image_order, jnp.asarray(frequencies()), image_query, image_key, image_value, gains[0], gains[1])

    from_y = [own[0]] + [shift(own[d], dy=d) for d in range(1, SIDE)]

    qt, kt, vt, bias = vmem_call(
        text_kernel,
        out_shape=[pltpu.VMEM((block, width), bf)] * 3 + [pltpu.VMEM((8, block), f32)],
        in_specs=[HB] * 6,
        out_specs=[VM] * 4,
        scratch_shapes=[
            pltpu.SMEM((1,), jnp.int32),
            pltpu.VMEM((block, width), bf),
            pltpu.VMEM((block, width), bf),
            pltpu.VMEM((1, HD), f32),
            pltpu.VMEM((1, HD), f32),
            pltpu.SemaphoreType.DMA((6,)),
        ],
        cost_estimate=pl.CostEstimate(flops=20_000_000, bytes_accessed=600_000, transcendentals=0),
        name="text",
    )(text_query, text_key, text_value, gains[2], gains[3], text_length)

    kv, q = vmem_call(
        pack_kernel,
        out_shape=[pltpu.VMEM((SIDE * rows, 2 * width), bf), pltpu.VMEM((SIDE * rows, width), bf)],
        in_specs=[VM] * SIDE + [VM],
        out_specs=[VM] * 2,
        name="pack",
    )(*from_y, bias)

    kvs = [kv] + [shift(kv, dx=d) for d in range(1, SIDE)]
    qs = [q] + [shift(q, dz=d) for d in range(1, SIDE)]

    parts = SIDE * SIDE
    out_rows = rows + text_rows // SIDE**3
    partial = pl.pallas_call(
        attend_kernel,
        out_shape=pltpu.VMEM((parts, out_rows, width + HD), bf),
        in_specs=[VM] * 12,
        out_specs=VM,
        name="attend",
    )(*kvs, *qs, qt, kt, vt, bias)

    groups = [[x * parts + i for i in range(parts)] for x in range(SIDE)]
    got = in_vmem(lax.all_to_all(partial, "seq", 0, 0, axis_index_groups=groups, tiled=True))

    return pl.pallas_call(
        combine_kernel,
        out_shape=[struct((rows, model), bf), struct((out_rows - rows, model), bf)],
        in_specs=[VM],
        out_specs=[VM] * 2,
        name="combine",
    )(got)


def solution(mesh):
    token = P(("req", "seq"), None)
    text = P("req", None)
    return jax.shard_map(
        lambda *args: tuple(local(*args)),
        mesh=mesh,
        in_specs=(token, token, token, text, text, text, P(), P(), P(), P(), P(("req", "seq")), P("req")),
        out_specs=(token, token),
        check_vma=False,
    )
```

```python
import jax
import jax.numpy as jnp
import numpy as np
from jax import lax
from jax.experimental import pallas as pl
from jax.experimental.pallas import tpu as pltpu
from jax.sharding import PartitionSpec as P

HD = 128
GRID_W = 64
SIDE = 4
EPS = 1e-06
MASKED = -1e30
SCALE = HD ** (-0.5)

VM = pl.BlockSpec(memory_space=pltpu.VMEM)
SM = pl.BlockSpec(memory_space=pltpu.SMEM)
HB = pl.BlockSpec(memory_space=pltpu.HBM)


def split_index(i):
    return i // (SIDE * SIDE), (i // SIDE) % SIDE, i % SIDE


def head_group(z, y):
    return ((z ^ (z >> 1)) & 1) * 2 + ((y ^ (y >> 1)) & 1)


def key_group(z, y):
    return (z >> 1) * 2 + (y >> 1)


HEAD_STEPS = ((0, 0, 0), (0, 1, 1), (0, 1, 0), (0, 0, 1))
QUERY_STEPS = ((0, 0, 0), (0, 3, 3), (0, 3, 0), (0, 0, 3))
KEY_STEPS = ((0, 0, 0), (2, 0, 0), (1, 0, 0), (3, 0, 0))


def exchange(value, step):
    pairs = []
    for i in range(SIDE**3):
        x, z, y = split_index(i)
        pairs.append((i, ((x ^ step[0]) * SIDE + (z ^ step[1])) * SIDE + (y ^ step[2])))
    return in_vmem(lax.ppermute(value, "seq", pairs))


def in_vmem(value):
    return pltpu.with_memory_space_constraint(value, pltpu.VMEM)


def vmem_call(kernel, **options):
    call = pl.pallas_call(kernel, **options)
    return lambda *args: jax.tree.map(in_vmem, call(*args))


def head_norm(x, gain):
    mean_square = jnp.mean(x * x, axis=-1, keepdims=True)
    return x * lax.rsqrt(mean_square + EPS) * gain


def frequencies():
    pair = np.arange(HD) // 2
    within = np.where(pair < 8, pair, np.where(pair < 36, pair - 8, pair - 36)).astype(np.float64)
    dim = np.where(pair < 8, 16.0, 56.0)
    return (10000.0 ** (-2.0 * within / dim)).astype(np.float32).reshape(1, HD)


def load(pairs, sems):
    copies = [pltpu.make_async_copy(src, dst, sems.at[i]) for i, (src, dst) in enumerate(pairs)]
    for c in copies:
        c.start()
    for c in copies:
        c.wait()


def prep_kernel(heads, half, order_h, freq_h, q_h, k_h, v_h, qg_h, kg_h, o0, o1, o2, o3, order, freq, q_in, k_in, v_in, qg, kg, q_s, k_s, sems):
    load(
        ((order_h, order), (freq_h, freq), (q_h, q_in), (k_h, k_in), (v_h, v_in), (qg_h, qg), (kg_h, kg)),
        sems,
    )
    rows = q_in.shape[0]
    lane = lax.broadcasted_iota(jnp.int32, (rows, HD), 1)
    row = lax.broadcasted_iota(jnp.int32, (rows, HD), 0)
    position = jnp.zeros((rows, HD), jnp.int32)
    for i in range(rows):
        position = jnp.where(row == i, order[i], position)
    inside = position & (half - 1)
    pair = lane >> 1
    coordinate = jnp.where(
        pair < 8,
        position >> (half.bit_length() - 1),
        jnp.where(pair < 36, inside >> (GRID_W.bit_length() - 1), inside & (GRID_W - 1)),
    )
    angle = coordinate.astype(jnp.float32) * freq[...]
    cosine = jnp.cos(angle)
    sine = jnp.sin(angle)
    even = (lane & 1) == 0
    sine = jnp.where(even, -sine, sine)
    blocks = [
        src[:, h * HD : (h + 1) * HD].astype(jnp.float32) for src in (q_in, k_in) for h in range(heads)
    ]
    whole = jnp.concatenate(blocks, axis=0)
    mean_square = jnp.mean(whole * whole, axis=-1, keepdims=True)
    whole = whole * lax.rsqrt(mean_square + EPS)
    for n in range(2 * heads):
        gain, dst, h = (qg, q_s, n) if n < heads else (kg, k_s, n - heads)
        x = whole[n * rows : (n + 1) * rows] * gain[...]
        partner = jnp.where(even, pltpu.roll(x, HD - 1, 1), pltpu.roll(x, 1, 1))
        dst[:, h * HD : (h + 1) * HD] = (x * cosine + partner * sine).astype(jnp.bfloat16)
    width = heads // SIDE * HD
    _, z, y = split_index(lax.axis_index("seq"))
    for step, out in zip(HEAD_STEPS, (o0, o1, o2, o3)):
        start = pl.multiple_of(head_group(z ^ step[1], y ^ step[2]) * width, HD)
        out[:, 0:width] = k_s[:, pl.ds(start, width)]
        out[:, width : 2 * width] = v_in[:, pl.ds(start, width)]
        out[:, 2 * width : 3 * width] = q_s[:, pl.ds(start, width)]


def pack_kernel(a0, a1, a2, a3, order_only, kv, q):
    rows = a0.shape[0]
    width = q.shape[1]
    for j, a in enumerate((a0, a1, a2, a3)):
        kv[j * rows : (j + 1) * rows, :] = a[:, : 2 * width]
        q[j * rows : (j + 1) * rows, :] = a[:, 2 * width :]


def text_kernel(q_h, k_h, v_h, qg_h, kg_h, length_h, q_out, k_out, v_out, bias, length, q_in, k_in, qg, kg, sems):
    block, width = q_in.shape
    x, z, y = split_index(lax.axis_index("seq"))
    group = key_group(z, y)
    cols = pl.ds(pl.multiple_of(head_group(z, y) * width, HD), width)
    q_rows = pl.ds(pl.multiple_of(x * block, block), block)
    k_rows = pl.ds(pl.multiple_of(group * block, block), block)
    load(
        (
            (length_h, length),
            (q_h.at[q_rows, cols], q_in),
            (k_h.at[k_rows, cols], k_in),
            (v_h.at[k_rows, cols], v_out),
            (qg_h, qg),
            (kg_h, kg),
        ),
        sems,
    )
    for src, gain, dst in ((q_in, qg, q_out), (k_in, kg, k_out)):
        g = gain[...]
        for h in range(width // HD):
            at = slice(h * HD, (h + 1) * HD)
            dst[:, at] = head_norm(src[:, at].astype(jnp.float32), g).astype(jnp.bfloat16)
    key = lax.broadcasted_iota(jnp.int32, bias.shape, 1) + group * block
    bias[...] = jnp.where(key < length[0], 0.0, MASKED)


def attend_kernel(kv0, kv1, kv2, kv3, q0, q1, q2, q3, qt, kt, vt, bias, out):
    kvs, qs = (kv0, kv1, kv2, kv3), (q0, q1, q2, q3)
    width = qt.shape[1]
    heads = width // HD
    text_keys = kt.shape[0]
    image_rows = SIDE * q0.shape[0]
    rows = image_rows + qt.shape[0]
    _, z, y = split_index(lax.axis_index("seq"))
    masked = bias[0:1, :]
    lane = lax.broadcasted_iota(jnp.int32, (rows, HD), 1)
    stats = jnp.zeros((rows, HD), jnp.float32)
    blended = []
    for h in range(heads):
        cols = slice(h * HD, (h + 1) * HD)
        vcols = slice(width + h * HD, width + (h + 1) * HD)
        query = jnp.concatenate([r[:, cols] for r in qs] + [qt[:, cols]], axis=0)
        key = jnp.concatenate([kt[:, cols]] + [r[:, cols] for r in kvs], axis=0)
        value = jnp.concatenate([vt[:, cols]] + [r[:, vcols] for r in kvs], axis=0)
        s = lax.dot_general(query, key, (((1,), (1,)), ((), ())), preferred_element_type=jnp.float32)
        s = jnp.concatenate([s[:, :text_keys] * SCALE + masked, s[:, text_keys:] * SCALE], axis=1)
        m = jnp.max(s, axis=1, keepdims=True)
        e = jnp.exp(s - m)
        l = jnp.sum(e, axis=1, keepdims=True)
        blended.append(jnp.dot(e.astype(jnp.bfloat16), value, preferred_element_type=jnp.float32))
        for first, value in ((h, m), (24 + h, l)):
            for piece in range(3 if first == h else 2):
                stats = jnp.where(lane == first + 8 * piece, value, stats)
                value = value - value.astype(jnp.bfloat16).astype(jnp.float32)
    blended.append(stats)
    for a, key_step in enumerate(QUERY_STEPS):
        for b, head_step in enumerate(HEAD_STEPS):
            i = a * SIDE + b
            there = (z ^ key_step[1] ^ head_step[1]) * SIDE + (y ^ key_step[2] ^ head_step[2])
            for c, part in enumerate(blended):
                cols = slice(c * HD, (c + 1) * HD)
                out[there, 0:8, cols] = part[i * 8 : (i + 1) * 8].astype(jnp.bfloat16)
                begin = image_rows + i * 8
                out[i, 8:16, cols] = part[begin : begin + 8].astype(jnp.bfloat16)


def combine_kernel(got, image_out, text_out):
    heads = (got.shape[2] - HD) // HD
    width = heads * HD
    half = image_out.shape[0]
    members = [[None] * SIDE for _ in range(SIDE)]
    for z in range(SIDE):
        for y in range(SIDE):
            members[key_group(z, y)][head_group(z, y)] = z * SIDE + y

    def stacked(key, cols):
        return jnp.concatenate([got[m, :, cols].astype(jnp.float32) for m in members[key]], axis=0)

    stats = [stacked(key, slice(width, width + HD)) for key in range(SIDE)]
    peaks = [s + pltpu.roll(s, HD - 8, 1) + pltpu.roll(s, HD - 16, 1) for s in stats]
    sums = [pltpu.roll(s, HD - 24, 1) + pltpu.roll(s, HD - 32, 1) for s in stats]
    top = jnp.maximum(jnp.maximum(peaks[0], peaks[1]), jnp.maximum(peaks[2], peaks[3]))
    factors = [jnp.exp(p - top) for p in peaks]
    total = factors[0] * sums[0] + factors[1] * sums[1] + factors[2] * sums[2] + factors[3] * sums[3]
    lane = lax.broadcasted_iota(jnp.int32, total.shape, 1)
    inverse = 1.0 / jnp.where(lane < heads, total, 1.0)
    weights = [f * inverse for f in factors]
    for h in range(heads):
        acc = 0.0
        for key in range(SIDE):
            acc = acc + stacked(key, slice(h * HD, (h + 1) * HD)) * weights[key][:, h : h + 1]
        for g in range(SIDE):
            cols = slice(g * width + h * HD, g * width + (h + 1) * HD)
            rows = acc[g * 2 * half : (g + 1) * 2 * half].astype(jnp.bfloat16)
            image_out[:, cols] = rows[:half]
            text_out[:, cols] = rows[half:]


def local(
    image_query,
    image_key,
    image_value,
    text_query,
    text_key,
    text_value,
    image_query_gain,
    image_key_gain,
    text_query_gain,
    text_key_gain,
    image_order,
    text_length,
):
    rows, model = image_query.shape
    heads = model // HD
    width = model // SIDE
    text_rows = text_query.shape[0]
    block = text_rows // SIDE
    half = rows * SIDE**3 // 2
    bf, f32 = jnp.bfloat16, jnp.float32
    struct = jax.ShapeDtypeStruct
    gains = [g.reshape(1, HD) for g in (image_query_gain, image_key_gain, text_query_gain, text_key_gain)]

    own = vmem_call(
        lambda *refs: prep_kernel(heads, half, *refs),
        out_shape=[pltpu.VMEM((rows, 3 * width), bf)] * SIDE,
        in_specs=[HB] * 7,
        out_specs=[VM] * SIDE,
        scratch_shapes=[
            pltpu.SMEM((rows,), jnp.int32),
            pltpu.VMEM((1, HD), f32),
            pltpu.VMEM((rows, model), bf),
            pltpu.VMEM((rows, model), bf),
            pltpu.VMEM((rows, model), bf),
            pltpu.VMEM((1, HD), f32),
            pltpu.VMEM((1, HD), f32),
            pltpu.VMEM((rows, model), bf),
            pltpu.VMEM((rows, model), bf),
            pltpu.SemaphoreType.DMA((7,)),
        ],
        name="prep",
    )(image_order, jnp.asarray(frequencies()), image_query, image_key, image_value, gains[0], gains[1])

    from_y = [own[0]] + [exchange(own[d], HEAD_STEPS[d]) for d in range(1, SIDE)]

    qt, kt, vt, bias = vmem_call(
        text_kernel,
        out_shape=[pltpu.VMEM((block, width), bf)] * 3 + [pltpu.VMEM((8, block), f32)],
        in_specs=[HB] * 6,
        out_specs=[VM] * 4,
        scratch_shapes=[
            pltpu.SMEM((1,), jnp.int32),
            pltpu.VMEM((block, width), bf),
            pltpu.VMEM((block, width), bf),
            pltpu.VMEM((1, HD), f32),
            pltpu.VMEM((1, HD), f32),
            pltpu.SemaphoreType.DMA((6,)),
        ],
        cost_estimate=pl.CostEstimate(flops=20_000_000, bytes_accessed=600_000, transcendentals=0),
        name="text",
    )(text_query, text_key, text_value, gains[2], gains[3], text_length)

    kv, q = vmem_call(
        pack_kernel,
        out_shape=[pltpu.VMEM((SIDE * rows, 2 * width), bf), pltpu.VMEM((SIDE * rows, width), bf)],
        in_specs=[VM] * SIDE + [VM],
        out_specs=[VM] * 2,
        name="pack",
    )(*from_y, bias)

    kvs = [kv] + [exchange(kv, step) for step in KEY_STEPS[1:]]
    qs = [q] + [exchange(q, step) for step in QUERY_STEPS[1:]]

    parts = SIDE * SIDE
    out_rows = rows + text_rows // SIDE**3
    partial = pl.pallas_call(
        attend_kernel,
        out_shape=pltpu.VMEM((parts, out_rows, width + HD), bf),
        in_specs=[VM] * 12,
        out_specs=VM,
        name="attend",
    )(*kvs, *qs, qt, kt, vt, bias)

    groups = [[x * parts + i for i in range(parts)] for x in range(SIDE)]
    got = in_vmem(lax.all_to_all(partial, "seq", 0, 0, axis_index_groups=groups, tiled=True))

    return pl.pallas_call(
        combine_kernel,
        out_shape=[struct((rows, model), bf), struct((out_rows - rows, model), bf)],
        in_specs=[VM],
        out_specs=[VM] * 2,
        name="combine",
    )(got)


def solution(mesh):
    token = P(("req", "seq"), None)
    text = P("req", None)
    return jax.shard_map(
        lambda *args: tuple(local(*args)),
        mesh=mesh,
        in_specs=(token, token, token, text, text, text, P(), P(), P(), P(), P(("req", "seq")), P("req")),
        out_specs=(token, token),
        check_vma=False,
    )
```

```python
import jax
import jax.numpy as jnp
import numpy as np
from jax import lax
from jax.experimental import pallas as pl
from jax.experimental.pallas import tpu as pltpu
from jax.sharding import PartitionSpec as P

HD = 128
GRID_W = 64
SIDE = 4
EPS = 1e-06
MASKED = -1e30
SCALE = HD ** (-0.5)

VM = pl.BlockSpec(memory_space=pltpu.VMEM)
SM = pl.BlockSpec(memory_space=pltpu.SMEM)
HB = pl.BlockSpec(memory_space=pltpu.HBM)


def split_index(i):
    return i // (SIDE * SIDE), (i // SIDE) % SIDE, i % SIDE


def head_group(z, y):
    return ((z ^ (z >> 1)) & 1) * 2 + ((y ^ (y >> 1)) & 1)


def key_group(z, y):
    return (z >> 1) * 2 + (y >> 1)


HEAD_STEPS = ((0, 0, 0), (0, 1, 1), (0, 1, 0), (0, 0, 1))
QUERY_STEPS = ((0, 0, 0), (0, 3, 0), (0, 0, 3), (0, 3, 3))
KEY_STEPS = ((0, 0, 0), (2, 0, 0), (1, 0, 0), (3, 0, 0))


def exchange(value, step):
    pairs = []
    for i in range(SIDE**3):
        x, z, y = split_index(i)
        pairs.append((i, ((x ^ step[0]) * SIDE + (z ^ step[1])) * SIDE + (y ^ step[2])))
    return in_vmem(lax.ppermute(value, "seq", pairs))


def in_vmem(value):
    return pltpu.with_memory_space_constraint(value, pltpu.VMEM)


def vmem_call(kernel, **options):
    call = pl.pallas_call(kernel, **options)
    return lambda *args: jax.tree.map(in_vmem, call(*args))


def head_norm(x, gain):
    mean_square = jnp.mean(x * x, axis=-1, keepdims=True)
    return x * lax.rsqrt(mean_square + EPS) * gain


def frequencies():
    pair = np.arange(HD) // 2
    within = np.where(pair < 8, pair, np.where(pair < 36, pair - 8, pair - 36)).astype(np.float64)
    dim = np.where(pair < 8, 16.0, 56.0)
    return (10000.0 ** (-2.0 * within / dim)).astype(np.float32).reshape(1, HD)


def load(pairs, sems):
    copies = [pltpu.make_async_copy(src, dst, sems.at[i]) for i, (src, dst) in enumerate(pairs)]
    for c in copies:
        c.start()
    for c in copies:
        c.wait()


def prep_kernel(heads, half, order_h, freq_h, q_h, k_h, v_h, qg_h, kg_h, o0, o1, o2, o3, order, freq, q_in, k_in, v_in, qg, kg, q_s, k_s, sems):
    load(
        ((order_h, order), (freq_h, freq), (q_h, q_in), (k_h, k_in), (v_h, v_in), (qg_h, qg), (kg_h, kg)),
        sems,
    )
    rows = q_in.shape[0]
    lane = lax.broadcasted_iota(jnp.int32, (rows, HD), 1)
    row = lax.broadcasted_iota(jnp.int32, (rows, HD), 0)
    position = jnp.zeros((rows, HD), jnp.int32)
    for i in range(rows):
        position = jnp.where(row == i, order[i], position)
    inside = position & (half - 1)
    pair = lane >> 1
    coordinate = jnp.where(
        pair < 8,
        position >> (half.bit_length() - 1),
        jnp.where(pair < 36, inside >> (GRID_W.bit_length() - 1), inside & (GRID_W - 1)),
    )
    angle = coordinate.astype(jnp.float32) * freq[...]
    cosine = jnp.cos(angle)
    sine = jnp.sin(angle)
    even = (lane & 1) == 0
    sine = jnp.where(even, -sine, sine)
    blocks = [
        src[:, h * HD : (h + 1) * HD].astype(jnp.float32) for src in (q_in, k_in) for h in range(heads)
    ]
    whole = jnp.concatenate(blocks, axis=0)
    mean_square = jnp.mean(whole * whole, axis=-1, keepdims=True)
    whole = whole * lax.rsqrt(mean_square + EPS)
    for n in range(2 * heads):
        gain, dst, h = (qg, q_s, n) if n < heads else (kg, k_s, n - heads)
        x = whole[n * rows : (n + 1) * rows] * gain[...]
        partner = jnp.where(even, pltpu.roll(x, HD - 1, 1), pltpu.roll(x, 1, 1))
        dst[:, h * HD : (h + 1) * HD] = (x * cosine + partner * sine).astype(jnp.bfloat16)
    width = heads // SIDE * HD
    _, z, y = split_index(lax.axis_index("seq"))
    for step, out in zip(HEAD_STEPS, (o0, o1, o2, o3)):
        start = pl.multiple_of(head_group(z ^ step[1], y ^ step[2]) * width, HD)
        out[:, 0:width] = k_s[:, pl.ds(start, width)]
        out[:, width : 2 * width] = v_in[:, pl.ds(start, width)]
        out[:, 2 * width : 3 * width] = q_s[:, pl.ds(start, width)]


def pack_kernel(a0, a1, a2, a3, order_only, kv, q):
    rows = a0.shape[0]
    width = q.shape[1]
    for j, a in enumerate((a0, a1, a2, a3)):
        kv[j * rows : (j + 1) * rows, :] = a[:, : 2 * width]
        q[j * rows : (j + 1) * rows, :] = a[:, 2 * width :]


def join_kernel(a, b, out):
    rows = a.shape[0]
    out[:rows, :] = a[...]
    out[rows:, :] = b[...]


def text_kernel(q_h, k_h, v_h, qg_h, kg_h, length_h, q_out, k_out, v_out, bias, length, q_in, k_in, qg, kg, sems):
    block, width = q_in.shape
    x, z, y = split_index(lax.axis_index("seq"))
    group = key_group(z, y)
    cols = pl.ds(pl.multiple_of(head_group(z, y) * width, HD), width)
    q_rows = pl.ds(pl.multiple_of(x * block, block), block)
    k_rows = pl.ds(pl.multiple_of(group * block, block), block)
    load(
        (
            (length_h, length),
            (q_h.at[q_rows, cols], q_in),
            (k_h.at[k_rows, cols], k_in),
            (v_h.at[k_rows, cols], v_out),
            (qg_h, qg),
            (kg_h, kg),
        ),
        sems,
    )
    for src, gain, dst in ((q_in, qg, q_out), (k_in, kg, k_out)):
        g = gain[...]
        for h in range(width // HD):
            at = slice(h * HD, (h + 1) * HD)
            dst[:, at] = head_norm(src[:, at].astype(jnp.float32), g).astype(jnp.bfloat16)
    key = lax.broadcasted_iota(jnp.int32, bias.shape, 1) + group * block
    bias[...] = jnp.where(key < length[0], 0.0, MASKED)


def attend_kernel(kv0, kv1, kv2, kv3, q0, q1, qt, kt, vt, bias, out):
    kvs, qs = (kv0, kv1, kv2, kv3), (q0, q1)
    width = qt.shape[1]
    heads = width // HD
    text_keys = kt.shape[0]
    image_rows = 2 * q0.shape[0]
    rows = image_rows + qt.shape[0]
    _, z, y = split_index(lax.axis_index("seq"))
    masked = bias[0:1, :]
    lane = lax.broadcasted_iota(jnp.int32, (rows, HD), 1)
    stats = jnp.zeros((rows, HD), jnp.float32)
    blended = []
    for h in range(heads):
        cols = slice(h * HD, (h + 1) * HD)
        vcols = slice(width + h * HD, width + (h + 1) * HD)
        query = jnp.concatenate([r[:, cols] for r in qs] + [qt[:, cols]], axis=0)
        key = jnp.concatenate([kt[:, cols]] + [r[:, cols] for r in kvs], axis=0)
        value = jnp.concatenate([vt[:, cols]] + [r[:, vcols] for r in kvs], axis=0)
        s = lax.dot_general(query, key, (((1,), (1,)), ((), ())), preferred_element_type=jnp.float32)
        s = jnp.concatenate([s[:, :text_keys] * SCALE + masked, s[:, text_keys:] * SCALE], axis=1)
        m = jnp.max(s, axis=1, keepdims=True)
        e = jnp.exp(s - m)
        l = jnp.sum(e, axis=1, keepdims=True)
        blended.append(jnp.dot(e.astype(jnp.bfloat16), value, preferred_element_type=jnp.float32))
        for first, value in ((h, m), (24 + h, l)):
            for piece in range(3 if first == h else 2):
                stats = jnp.where(lane == first + 8 * piece, value, stats)
                value = value - value.astype(jnp.bfloat16).astype(jnp.float32)
    blended.append(stats)
    for a, key_step in enumerate(QUERY_STEPS):
        for b, head_step in enumerate(HEAD_STEPS):
            i = a * SIDE + b
            there = (z ^ key_step[1] ^ head_step[1]) * SIDE + (y ^ key_step[2] ^ head_step[2])
            for c, part in enumerate(blended):
                cols = slice(c * HD, (c + 1) * HD)
                out[there, 0:8, cols] = part[i * 8 : (i + 1) * 8].astype(jnp.bfloat16)
                begin = image_rows + i * 8
                out[i, 8:16, cols] = part[begin : begin + 8].astype(jnp.bfloat16)


def combine_kernel(got, image_out, text_out):
    heads = (got.shape[2] - HD) // HD
    width = heads * HD
    half = image_out.shape[0]
    members = [[None] * SIDE for _ in range(SIDE)]
    for z in range(SIDE):
        for y in range(SIDE):
            members[key_group(z, y)][head_group(z, y)] = z * SIDE + y

    def stacked(key, cols):
        return jnp.concatenate([got[m, :, cols].astype(jnp.float32) for m in members[key]], axis=0)

    stats = [stacked(key, slice(width, width + HD)) for key in range(SIDE)]
    peaks = [s + pltpu.roll(s, HD - 8, 1) + pltpu.roll(s, HD - 16, 1) for s in stats]
    sums = [pltpu.roll(s, HD - 24, 1) + pltpu.roll(s, HD - 32, 1) for s in stats]
    top = jnp.maximum(jnp.maximum(peaks[0], peaks[1]), jnp.maximum(peaks[2], peaks[3]))
    factors = [jnp.exp(p - top) for p in peaks]
    total = factors[0] * sums[0] + factors[1] * sums[1] + factors[2] * sums[2] + factors[3] * sums[3]
    lane = lax.broadcasted_iota(jnp.int32, total.shape, 1)
    inverse = 1.0 / jnp.where(lane < heads, total, 1.0)
    weights = [f * inverse for f in factors]
    for h in range(heads):
        acc = 0.0
        for key in range(SIDE):
            acc = acc + stacked(key, slice(h * HD, (h + 1) * HD)) * weights[key][:, h : h + 1]
        for g in range(SIDE):
            cols = slice(g * width + h * HD, g * width + (h + 1) * HD)
            rows = acc[g * 2 * half : (g + 1) * 2 * half].astype(jnp.bfloat16)
            image_out[:, cols] = rows[:half]
            text_out[:, cols] = rows[half:]


def local(
    image_query,
    image_key,
    image_value,
    text_query,
    text_key,
    text_value,
    image_query_gain,
    image_key_gain,
    text_query_gain,
    text_key_gain,
    image_order,
    text_length,
):
    rows, model = image_query.shape
    heads = model // HD
    width = model // SIDE
    text_rows = text_query.shape[0]
    block = text_rows // SIDE
    half = rows * SIDE**3 // 2
    bf, f32 = jnp.bfloat16, jnp.float32
    struct = jax.ShapeDtypeStruct
    gains = [g.reshape(1, HD) for g in (image_query_gain, image_key_gain, text_query_gain, text_key_gain)]

    own = vmem_call(
        lambda *refs: prep_kernel(heads, half, *refs),
        out_shape=[pltpu.VMEM((rows, 3 * width), bf)] * SIDE,
        in_specs=[HB] * 7,
        out_specs=[VM] * SIDE,
        scratch_shapes=[
            pltpu.SMEM((rows,), jnp.int32),
            pltpu.VMEM((1, HD), f32),
            pltpu.VMEM((rows, model), bf),
            pltpu.VMEM((rows, model), bf),
            pltpu.VMEM((rows, model), bf),
            pltpu.VMEM((1, HD), f32),
            pltpu.VMEM((1, HD), f32),
            pltpu.VMEM((rows, model), bf),
            pltpu.VMEM((rows, model), bf),
            pltpu.SemaphoreType.DMA((7,)),
        ],
        name="prep",
    )(image_order, jnp.asarray(frequencies()), image_query, image_key, image_value, gains[0], gains[1])

    from_y = [own[0]] + [exchange(own[d], HEAD_STEPS[d]) for d in range(1, SIDE)]

    qt, kt, vt, bias = vmem_call(
        text_kernel,
        out_shape=[pltpu.VMEM((block, width), bf)] * 3 + [pltpu.VMEM((8, block), f32)],
        in_specs=[HB] * 6,
        out_specs=[VM] * 4,
        scratch_shapes=[
            pltpu.SMEM((1,), jnp.int32),
            pltpu.VMEM((block, width), bf),
            pltpu.VMEM((block, width), bf),
            pltpu.VMEM((1, HD), f32),
            pltpu.VMEM((1, HD), f32),
            pltpu.SemaphoreType.DMA((6,)),
        ],
        cost_estimate=pl.CostEstimate(flops=20_000_000, bytes_accessed=600_000, transcendentals=0),
        name="text",
    )(text_query, text_key, text_value, gains[2], gains[3], text_length)

    kv, q = vmem_call(
        pack_kernel,
        out_shape=[pltpu.VMEM((SIDE * rows, 2 * width), bf), pltpu.VMEM((SIDE * rows, width), bf)],
        in_specs=[VM] * SIDE + [VM],
        out_specs=[VM] * 2,
        name="pack",
    )(*from_y, bias)

    with jax.named_scope("query_first"):
        q_next = exchange(q, QUERY_STEPS[1])
    kvs = [kv]
    for i in range(1, SIDE):
        with jax.named_scope(f"keys_{i}"):
            kvs.append(exchange(kv, KEY_STEPS[i]))
    q_two = vmem_call(
        join_kernel,
        out_shape=pltpu.VMEM((2 * SIDE * rows, width), bf),
        in_specs=[VM] * 2,
        out_specs=VM,
        name="join",
    )(q, q_next)
    with jax.named_scope("query_second"):
        q_last = exchange(q_two, QUERY_STEPS[2])

    parts = SIDE * SIDE
    out_rows = rows + text_rows // SIDE**3
    partial = pl.pallas_call(
        attend_kernel,
        out_shape=pltpu.VMEM((parts, out_rows, width + HD), bf),
        in_specs=[VM] * 10,
        out_specs=VM,
        name="attend",
    )(*kvs, q_two, q_last, qt, kt, vt, bias)

    groups = [[x * parts + i for i in range(parts)] for x in range(SIDE)]
    got = in_vmem(lax.all_to_all(partial, "seq", 0, 0, axis_index_groups=groups, tiled=True))

    return pl.pallas_call(
        combine_kernel,
        out_shape=[struct((rows, model), bf), struct((out_rows - rows, model), bf)],
        in_specs=[VM],
        out_specs=[VM] * 2,
        name="combine",
    )(got)


def solution(mesh):
    token = P(("req", "seq"), None)
    text = P("req", None)
    return jax.shard_map(
        lambda *args: tuple(local(*args)),
        mesh=mesh,
        in_specs=(token, token, token, text, text, text, P(), P(), P(), P(), P(("req", "seq")), P("req")),
        out_specs=(token, token),
        check_vma=False,
    )
```

```python
import jax
import jax.numpy as jnp
import numpy as np
from jax import lax
from jax.experimental import pallas as pl
from jax.experimental.pallas import tpu as pltpu
from jax.sharding import PartitionSpec as P

HD = 128
GRID_W = 64
SIDE = 4
EPS = 1e-06
MASKED = -1e30
SCALE = HD ** (-0.5)

VM = pl.BlockSpec(memory_space=pltpu.VMEM)
SM = pl.BlockSpec(memory_space=pltpu.SMEM)
HB = pl.BlockSpec(memory_space=pltpu.HBM)


def split_index(i):
    return i // (SIDE * SIDE), (i // SIDE) % SIDE, i % SIDE


def head_group(z, y):
    return ((z ^ (z >> 1)) & 1) * 2 + ((y ^ (y >> 1)) & 1)


def key_group(z, y):
    return (z >> 1) * 2 + (y >> 1)


HEAD_STEPS = ((0, 0, 0), (0, 1, 1), (0, 1, 0), (0, 0, 1))
QUERY_STEPS = ((0, 0, 0), (0, 3, 0), (0, 0, 3), (0, 3, 3))
KEY_STEPS = ((0, 0, 0), (1, 0, 0), (3, 0, 0), (2, 0, 0))


def exchange(value, step):
    pairs = []
    for i in range(SIDE**3):
        x, z, y = split_index(i)
        pairs.append((i, ((x ^ step[0]) * SIDE + (z ^ step[1])) * SIDE + (y ^ step[2])))
    return in_vmem(lax.ppermute(value, "seq", pairs))


def in_vmem(value):
    return pltpu.with_memory_space_constraint(value, pltpu.VMEM)


def vmem_call(kernel, **options):
    call = pl.pallas_call(kernel, **options)
    return lambda *args: jax.tree.map(in_vmem, call(*args))


def head_norm(x, gain):
    mean_square = jnp.mean(x * x, axis=-1, keepdims=True)
    return x * lax.rsqrt(mean_square + EPS) * gain


def frequencies():
    pair = np.arange(HD) // 2
    within = np.where(pair < 8, pair, np.where(pair < 36, pair - 8, pair - 36)).astype(np.float64)
    dim = np.where(pair < 8, 16.0, 56.0)
    return (10000.0 ** (-2.0 * within / dim)).astype(np.float32).reshape(1, HD)


def load(pairs, sems):
    copies = [pltpu.make_async_copy(src, dst, sems.at[i]) for i, (src, dst) in enumerate(pairs)]
    for c in copies:
        c.start()
    for c in copies:
        c.wait()


def prep_kernel(heads, half, order_h, freq_h, q_h, k_h, v_h, qg_h, kg_h, o0, o1, o2, o3, order, freq, q_in, k_in, v_in, qg, kg, q_s, k_s, sems):
    load(
        ((order_h, order), (freq_h, freq), (q_h, q_in), (k_h, k_in), (v_h, v_in), (qg_h, qg), (kg_h, kg)),
        sems,
    )
    rows = q_in.shape[0]
    lane = lax.broadcasted_iota(jnp.int32, (rows, HD), 1)
    row = lax.broadcasted_iota(jnp.int32, (rows, HD), 0)
    position = jnp.zeros((rows, HD), jnp.int32)
    for i in range(rows):
        position = jnp.where(row == i, order[i], position)
    inside = position & (half - 1)
    pair = lane >> 1
    coordinate = jnp.where(
        pair < 8,
        position >> (half.bit_length() - 1),
        jnp.where(pair < 36, inside >> (GRID_W.bit_length() - 1), inside & (GRID_W - 1)),
    )
    angle = coordinate.astype(jnp.float32) * freq[...]
    cosine = jnp.cos(angle)
    sine = jnp.sin(angle)
    even = (lane & 1) == 0
    sine = jnp.where(even, -sine, sine)
    blocks = [
        src[:, h * HD : (h + 1) * HD].astype(jnp.float32) for src in (q_in, k_in) for h in range(heads)
    ]
    whole = jnp.concatenate(blocks, axis=0)
    mean_square = jnp.mean(whole * whole, axis=-1, keepdims=True)
    whole = whole * lax.rsqrt(mean_square + EPS)
    for n in range(2 * heads):
        gain, dst, h = (qg, q_s, n) if n < heads else (kg, k_s, n - heads)
        x = whole[n * rows : (n + 1) * rows] * gain[...]
        partner = jnp.where(even, pltpu.roll(x, HD - 1, 1), pltpu.roll(x, 1, 1))
        dst[:, h * HD : (h + 1) * HD] = (x * cosine + partner * sine).astype(jnp.bfloat16)
    width = heads // SIDE * HD
    _, z, y = split_index(lax.axis_index("seq"))
    for step, out in zip(HEAD_STEPS, (o0, o1, o2, o3)):
        start = pl.multiple_of(head_group(z ^ step[1], y ^ step[2]) * width, HD)
        out[:, 0:width] = k_s[:, pl.ds(start, width)]
        out[:, width : 2 * width] = v_in[:, pl.ds(start, width)]
        out[:, 2 * width : 3 * width] = q_s[:, pl.ds(start, width)]


def pack_kernel(a0, a1, a2, a3, order_only, kv, q):
    rows = a0.shape[0]
    width = q.shape[1]
    for j, a in enumerate((a0, a1, a2, a3)):
        kv[j * rows : (j + 1) * rows, :] = a[:, : 2 * width]
        q[j * rows : (j + 1) * rows, :] = a[:, 2 * width :]


def join_kernel(a, b, out):
    rows = a.shape[0]
    out[:rows, :] = a[...]
    out[rows:, :] = b[...]


def text_kernel(q_h, k_h, v_h, qg_h, kg_h, length_h, q_out, k_out, v_out, bias, length, q_in, k_in, qg, kg, sems):
    block, width = q_in.shape
    x, z, y = split_index(lax.axis_index("seq"))
    group = key_group(z, y)
    cols = pl.ds(pl.multiple_of(head_group(z, y) * width, HD), width)
    q_rows = pl.ds(pl.multiple_of(x * block, block), block)
    k_rows = pl.ds(pl.multiple_of(group * block, block), block)
    load(
        (
            (length_h, length),
            (q_h.at[q_rows, cols], q_in),
            (k_h.at[k_rows, cols], k_in),
            (v_h.at[k_rows, cols], v_out),
            (qg_h, qg),
            (kg_h, kg),
        ),
        sems,
    )
    for src, gain, dst in ((q_in, qg, q_out), (k_in, kg, k_out)):
        g = gain[...]
        for h in range(width // HD):
            at = slice(h * HD, (h + 1) * HD)
            dst[:, at] = head_norm(src[:, at].astype(jnp.float32), g).astype(jnp.bfloat16)
    key = lax.broadcasted_iota(jnp.int32, bias.shape, 1) + group * block
    bias[...] = jnp.where(key < length[0], 0.0, MASKED)


def attend_kernel(kv0, kv1, q0, q1, qt, kt, vt, bias, out):
    kvs, qs = (kv0, kv1), (q0, q1)
    width = qt.shape[1]
    heads = width // HD
    text_keys = kt.shape[0]
    image_rows = 2 * q0.shape[0]
    rows = image_rows + qt.shape[0]
    _, z, y = split_index(lax.axis_index("seq"))
    masked = bias[0:1, :]
    lane = lax.broadcasted_iota(jnp.int32, (rows, HD), 1)
    stats = jnp.zeros((rows, HD), jnp.float32)
    blended = []
    for h in range(heads):
        cols = slice(h * HD, (h + 1) * HD)
        vcols = slice(width + h * HD, width + (h + 1) * HD)
        query = jnp.concatenate([r[:, cols] for r in qs] + [qt[:, cols]], axis=0)
        key = jnp.concatenate([kt[:, cols]] + [r[:, cols] for r in kvs], axis=0)
        value = jnp.concatenate([vt[:, cols]] + [r[:, vcols] for r in kvs], axis=0)
        s = lax.dot_general(query, key, (((1,), (1,)), ((), ())), preferred_element_type=jnp.float32)
        s = jnp.concatenate([s[:, :text_keys] * SCALE + masked, s[:, text_keys:] * SCALE], axis=1)
        m = jnp.max(s, axis=1, keepdims=True)
        e = jnp.exp(s - m)
        l = jnp.sum(e, axis=1, keepdims=True)
        blended.append(jnp.dot(e.astype(jnp.bfloat16), value, preferred_element_type=jnp.float32))
        for first, value in ((h, m), (24 + h, l)):
            for piece in range(3 if first == h else 2):
                stats = jnp.where(lane == first + 8 * piece, value, stats)
                value = value - value.astype(jnp.bfloat16).astype(jnp.float32)
    blended.append(stats)
    for a, key_step in enumerate(QUERY_STEPS):
        for b, head_step in enumerate(HEAD_STEPS):
            i = a * SIDE + b
            there = (z ^ key_step[1] ^ head_step[1]) * SIDE + (y ^ key_step[2] ^ head_step[2])
            for c, part in enumerate(blended):
                cols = slice(c * HD, (c + 1) * HD)
                out[there, 0:8, cols] = part[i * 8 : (i + 1) * 8].astype(jnp.bfloat16)
                begin = image_rows + i * 8
                out[i, 8:16, cols] = part[begin : begin + 8].astype(jnp.bfloat16)


def combine_kernel(got, image_out, text_out):
    heads = (got.shape[2] - HD) // HD
    width = heads * HD
    half = image_out.shape[0]
    members = [[None] * SIDE for _ in range(SIDE)]
    for z in range(SIDE):
        for y in range(SIDE):
            members[key_group(z, y)][head_group(z, y)] = z * SIDE + y

    def stacked(key, cols):
        return jnp.concatenate([got[m, :, cols].astype(jnp.float32) for m in members[key]], axis=0)

    stats = [stacked(key, slice(width, width + HD)) for key in range(SIDE)]
    peaks = [s + pltpu.roll(s, HD - 8, 1) + pltpu.roll(s, HD - 16, 1) for s in stats]
    sums = [pltpu.roll(s, HD - 24, 1) + pltpu.roll(s, HD - 32, 1) for s in stats]
    top = jnp.maximum(jnp.maximum(peaks[0], peaks[1]), jnp.maximum(peaks[2], peaks[3]))
    factors = [jnp.exp(p - top) for p in peaks]
    total = factors[0] * sums[0] + factors[1] * sums[1] + factors[2] * sums[2] + factors[3] * sums[3]
    lane = lax.broadcasted_iota(jnp.int32, total.shape, 1)
    inverse = 1.0 / jnp.where(lane < heads, total, 1.0)
    weights = [f * inverse for f in factors]
    for h in range(heads):
        acc = 0.0
        for key in range(SIDE):
            acc = acc + stacked(key, slice(h * HD, (h + 1) * HD)) * weights[key][:, h : h + 1]
        for g in range(SIDE):
            cols = slice(g * width + h * HD, g * width + (h + 1) * HD)
            rows = acc[g * 2 * half : (g + 1) * 2 * half].astype(jnp.bfloat16)
            image_out[:, cols] = rows[:half]
            text_out[:, cols] = rows[half:]


def local(
    image_query,
    image_key,
    image_value,
    text_query,
    text_key,
    text_value,
    image_query_gain,
    image_key_gain,
    text_query_gain,
    text_key_gain,
    image_order,
    text_length,
):
    rows, model = image_query.shape
    heads = model // HD
    width = model // SIDE
    text_rows = text_query.shape[0]
    block = text_rows // SIDE
    half = rows * SIDE**3 // 2
    bf, f32 = jnp.bfloat16, jnp.float32
    struct = jax.ShapeDtypeStruct
    gains = [g.reshape(1, HD) for g in (image_query_gain, image_key_gain, text_query_gain, text_key_gain)]

    own = vmem_call(
        lambda *refs: prep_kernel(heads, half, *refs),
        out_shape=[pltpu.VMEM((rows, 3 * width), bf)] * SIDE,
        in_specs=[HB] * 7,
        out_specs=[VM] * SIDE,
        scratch_shapes=[
            pltpu.SMEM((rows,), jnp.int32),
            pltpu.VMEM((1, HD), f32),
            pltpu.VMEM((rows, model), bf),
            pltpu.VMEM((rows, model), bf),
            pltpu.VMEM((rows, model), bf),
            pltpu.VMEM((1, HD), f32),
            pltpu.VMEM((1, HD), f32),
            pltpu.VMEM((rows, model), bf),
            pltpu.VMEM((rows, model), bf),
            pltpu.SemaphoreType.DMA((7,)),
        ],
        name="prep",
    )(image_order, jnp.asarray(frequencies()), image_query, image_key, image_value, gains[0], gains[1])

    from_y = [own[0]] + [exchange(own[d], HEAD_STEPS[d]) for d in range(1, SIDE)]

    qt, kt, vt, bias = vmem_call(
        text_kernel,
        out_shape=[pltpu.VMEM((block, width), bf)] * 3 + [pltpu.VMEM((8, block), f32)],
        in_specs=[HB] * 6,
        out_specs=[VM] * 4,
        scratch_shapes=[
            pltpu.SMEM((1,), jnp.int32),
            pltpu.VMEM((block, width), bf),
            pltpu.VMEM((block, width), bf),
            pltpu.VMEM((1, HD), f32),
            pltpu.VMEM((1, HD), f32),
            pltpu.SemaphoreType.DMA((6,)),
        ],
        cost_estimate=pl.CostEstimate(flops=20_000_000, bytes_accessed=600_000, transcendentals=0),
        name="text",
    )(text_query, text_key, text_value, gains[2], gains[3], text_length)

    kv, q = vmem_call(
        pack_kernel,
        out_shape=[pltpu.VMEM((SIDE * rows, 2 * width), bf), pltpu.VMEM((SIDE * rows, width), bf)],
        in_specs=[VM] * SIDE + [VM],
        out_specs=[VM] * 2,
        name="pack",
    )(*from_y, bias)

    def join(a, b):
        return vmem_call(
            join_kernel,
            out_shape=pltpu.VMEM((a.shape[0] + b.shape[0], a.shape[1]), a.dtype),
            in_specs=[VM] * 2,
            out_specs=VM,
            name="join",
        )(a, b)

    kv_next = exchange(kv, KEY_STEPS[1])
    q_next = exchange(q, QUERY_STEPS[1])
    kv_two = join(kv, kv_next)
    kv_last = exchange(kv_two, KEY_STEPS[2])
    q_two = join(q, q_next)
    q_last = exchange(q_two, QUERY_STEPS[2])

    parts = SIDE * SIDE
    out_rows = rows + text_rows // SIDE**3
    partial = pl.pallas_call(
        attend_kernel,
        out_shape=pltpu.VMEM((parts, out_rows, width + HD), bf),
        in_specs=[VM] * 8,
        out_specs=VM,
        name="attend",
    )(kv_two, kv_last, q_two, q_last, qt, kt, vt, bias)

    groups = [[x * parts + i for i in range(parts)] for x in range(SIDE)]
    got = in_vmem(lax.all_to_all(partial, "seq", 0, 0, axis_index_groups=groups, tiled=True))

    return pl.pallas_call(
        combine_kernel,
        out_shape=[struct((rows, model), bf), struct((out_rows - rows, model), bf)],
        in_specs=[VM],
        out_specs=[VM] * 2,
        name="combine",
    )(got)


def whole(*args):
    return tuple(local(*args))


def solution(mesh):
    token = P(("req", "seq"), None)
    text = P("req", None)
    return jax.shard_map(
        whole,
        mesh=mesh,
        in_specs=(token, token, token, text, text, text, P(), P(), P(), P(), P(("req", "seq")), P("req")),
        out_specs=(token, token),
        check_vma=False,
    )
```

```python
import jax
import jax.numpy as jnp
import numpy as np
from jax import lax
from jax.experimental import pallas as pl
from jax.experimental.pallas import tpu as pltpu
from jax.sharding import PartitionSpec as P

HD = 128
GRID_W = 64
SIDE = 4
EPS = 1e-06
MASKED = -1e30
SCALE = HD ** (-0.5)
LOG2E = 1.4426950408889634

VM = pl.BlockSpec(memory_space=pltpu.VMEM)
SM = pl.BlockSpec(memory_space=pltpu.SMEM)
HB = pl.BlockSpec(memory_space=pltpu.HBM)


def split_index(i):
    return i // (SIDE * SIDE), (i // SIDE) % SIDE, i % SIDE


def parity(i):
    return (i ^ (i >> 1)) & 1


def head_group(z, y):
    return parity(z) * 2 + parity(y)


def key_group(x, z):
    return parity(x) * 2 + (z >> 1)


def member(x, z, y):
    return parity(x) * 8 + z * 2 + parity(y)


HEAD_STEPS = ((0, 0, 0), (0, 1, 1), (0, 1, 0), (0, 0, 1))
QUERY_STEPS = ((0, 0, 0), (0, 3, 0), (1, 0, 0), (1, 3, 0))
KEY_STEPS = ((0, 0, 0), (3, 0, 3), (3, 0, 0), (0, 0, 3))


def query_groups():
    groups = {}
    for i in range(SIDE**3):
        x, z, y = split_index(i)
        groups.setdefault((x >> 1, y >> 1), {})[member(x, z, y)] = i
    return [[g[j] for j in range(len(g))] for g in groups.values()]


def exchange(value, step):
    pairs = []
    for i in range(SIDE**3):
        x, z, y = split_index(i)
        pairs.append((i, ((x ^ step[0]) * SIDE + (z ^ step[1])) * SIDE + (y ^ step[2])))
    return in_vmem(lax.ppermute(value, "seq", pairs))


def in_vmem(value):
    return pltpu.with_memory_space_constraint(value, pltpu.VMEM)


def vmem_call(kernel, **options):
    call = pl.pallas_call(kernel, **options)
    return lambda *args: jax.tree.map(in_vmem, call(*args))


def head_norm(x, gain):
    mean_square = jnp.mean(x * x, axis=-1, keepdims=True)
    return x * lax.rsqrt(mean_square + EPS) * gain


def frequencies():
    pair = np.arange(HD) // 2
    within = np.where(pair < 8, pair, np.where(pair < 36, pair - 8, pair - 36)).astype(np.float64)
    dim = np.where(pair < 8, 16.0, 56.0)
    return (10000.0 ** (-2.0 * within / dim)).astype(np.float32).reshape(1, HD)


def load(pairs, sems):
    copies = [pltpu.make_async_copy(src, dst, sems.at[i]) for i, (src, dst) in enumerate(pairs)]
    for c in copies:
        c.start()
    for c in copies:
        c.wait()


def prep_kernel(heads, half, order_h, freq_h, q_h, k_h, v_h, qg_h, kg_h, o0, o1, o2, o3, order, freq, q_in, k_in, v_in, qg, kg, q_s, k_s, sems):
    load(
        ((order_h, order), (freq_h, freq), (q_h, q_in), (k_h, k_in), (v_h, v_in), (qg_h, qg), (kg_h, kg)),
        sems,
    )
    rows = q_in.shape[0]
    lane = lax.broadcasted_iota(jnp.int32, (rows, HD), 1)
    row = lax.broadcasted_iota(jnp.int32, (rows, HD), 0)
    position = jnp.zeros((rows, HD), jnp.int32)
    for i in range(rows):
        position = jnp.where(row == i, order[i], position)
    inside = position & (half - 1)
    pair = lane >> 1
    coordinate = jnp.where(
        pair < 8,
        position >> (half.bit_length() - 1),
        jnp.where(pair < 36, inside >> (GRID_W.bit_length() - 1), inside & (GRID_W - 1)),
    )
    angle = coordinate.astype(jnp.float32) * freq[...]
    cosine = jnp.cos(angle)
    sine = jnp.sin(angle)
    even = (lane & 1) == 0
    sine = jnp.where(even, -sine, sine)
    blocks = [
        src[:, h * HD : (h + 1) * HD].astype(jnp.float32) for src in (q_in, k_in) for h in range(heads)
    ]
    whole = jnp.concatenate(blocks, axis=0)
    mean_square = jnp.mean(whole * whole, axis=-1, keepdims=True)
    whole = whole * lax.rsqrt(mean_square + EPS)
    for n in range(2 * heads):
        gain, dst, h = (qg, q_s, n) if n < heads else (kg, k_s, n - heads)
        x = whole[n * rows : (n + 1) * rows] * gain[...]
        partner = jnp.where(even, pltpu.roll(x, HD - 1, 1), pltpu.roll(x, 1, 1))
        dst[:, h * HD : (h + 1) * HD] = (x * cosine + partner * sine).astype(jnp.bfloat16)
    width = heads // SIDE * HD
    _, z, y = split_index(lax.axis_index("seq"))
    for step, out in zip(HEAD_STEPS, (o0, o1, o2, o3)):
        start = pl.multiple_of(head_group(z ^ step[1], y ^ step[2]) * width, HD)
        out[:, 0:width] = k_s[:, pl.ds(start, width)]
        out[:, width : 2 * width] = v_in[:, pl.ds(start, width)]
        out[:, 2 * width : 3 * width] = q_s[:, pl.ds(start, width)]


def pack_kernel(a0, a1, a2, a3, order_only, kv, q):
    rows = a0.shape[0]
    width = q.shape[1]
    for j, a in enumerate((a0, a1, a2, a3)):
        kv[j * rows : (j + 1) * rows, :] = a[:, : 2 * width]
        q[j * rows : (j + 1) * rows, :] = a[:, 2 * width :]


def join_kernel(a, b, out):
    rows = a.shape[0]
    out[:rows, :] = a[...]
    out[rows:, :] = b[...]


def text_kernel(q_h, k_h, v_h, qg_h, kg_h, length_h, q_out, k_out, v_out, bias, length, q_in, k_in, qg, kg, sems):
    block, width = k_in.shape
    x, z, y = split_index(lax.axis_index("seq"))
    group = key_group(x, z)
    cols = pl.ds(pl.multiple_of(head_group(z, y) * width, HD), width)
    k_rows = pl.ds(pl.multiple_of(group * block, block), block)
    pieces = [
        (length_h, length),
        (k_h.at[k_rows, cols], k_in),
        (v_h.at[k_rows, cols], v_out),
        (qg_h, qg),
        (kg_h, kg),
    ]
    own = q_in.shape[1]
    for j in range(q_in.shape[0]):
        px, jz, py = j >> 3, (j >> 1) & 3, j & 1
        jx = (x & 2) + (px ^ (x >> 1))
        jy = (y & 2) + (py ^ (y >> 1))
        start = ((jx * SIDE + jz) * SIDE + jy) * own
        pieces.append((q_h.at[pl.ds(pl.multiple_of(start, own), own), cols], q_in.at[j]))
    load(pieces, sems)
    for gain, dst in ((qg, q_out), (kg, k_out)):
        g = gain[...]
        for h in range(width // HD):
            at = slice(h * HD, (h + 1) * HD)
            if dst is q_out:
                rows = q_in[:, :, at].astype(jnp.float32).reshape(block, HD)
            else:
                rows = k_in[:, at].astype(jnp.float32)
            dst[:, at] = head_norm(rows, g).astype(jnp.bfloat16)
    key = lax.broadcasted_iota(jnp.int32, bias.shape, 1) + group * block
    bias[...] = jnp.where(key < length[0], 0.0, MASKED)


def attend_kernel(kv0, kv1, kv2, kv3, q0, q1, qt, kt, vt, bias, out):
    kvs, qs = (kv0, kv1, kv2, kv3), (q0, q1)
    width = qt.shape[1]
    heads = width // HD
    text_keys = kt.shape[0]
    image_rows = 2 * q0.shape[0]
    rows = image_rows + qt.shape[0]
    x, z, y = split_index(lax.axis_index("seq"))
    masked = bias[0:1, :]
    lane = lax.broadcasted_iota(jnp.int32, (rows, HD), 1)
    stats = jnp.zeros((rows, HD), jnp.float32)
    blended = []
    for h in range(heads):
        cols = slice(h * HD, (h + 1) * HD)
        vcols = slice(width + h * HD, width + (h + 1) * HD)
        query = jnp.concatenate([r[:, cols] for r in qs] + [qt[:, cols]], axis=0)
        key = jnp.concatenate([kt[:, cols]] + [r[:, cols] for r in kvs], axis=0)
        value = jnp.concatenate([vt[:, cols]] + [r[:, vcols] for r in kvs], axis=0)
        s = lax.dot_general(query, key, (((1,), (1,)), ((), ())), preferred_element_type=jnp.float32)
        s = jnp.concatenate([s[:, :text_keys] + masked, s[:, text_keys:]], axis=1)
        m = jnp.max(s, axis=1, keepdims=True)
        e = jnp.exp2((s - m) * (SCALE * LOG2E))
        m = m * SCALE
        l = jnp.sum(e, axis=1, keepdims=True)
        blended.append(jnp.dot(e.astype(jnp.bfloat16), value, preferred_element_type=jnp.float32))
        for first, value in ((h, m), (24 + h, l)):
            for piece in range(3 if first == h else 2):
                stats = jnp.where(lane == first + 8 * piece, value, stats)
                value = value - value.astype(jnp.bfloat16).astype(jnp.float32)
    blended.append(stats)
    for a, key_step in enumerate(QUERY_STEPS):
        for b, head_step in enumerate(HEAD_STEPS):
            i = a * SIDE + b
            there = member(x ^ key_step[0], z ^ key_step[1] ^ head_step[1], y ^ head_step[2])
            for c, part in enumerate(blended):
                cols = slice(c * HD, (c + 1) * HD)
                out[there, 0:8, cols] = part[i * 8 : (i + 1) * 8].astype(jnp.bfloat16)
                begin = image_rows + i * 8
                out[i, 8:16, cols] = part[begin : begin + 8].astype(jnp.bfloat16)


def combine_kernel(got, image_out, text_out):
    heads = (got.shape[2] - HD) // HD
    width = heads * HD
    half = image_out.shape[0]
    members = [[None] * SIDE for _ in range(SIDE)]
    for j in range(got.shape[0]):
        px, z, py = j >> 3, (j >> 1) & 3, j & 1
        members[px * 2 + (z >> 1)][parity(z) * 2 + py] = j

    def stacked(key, cols):
        return jnp.concatenate([got[m, :, cols].astype(jnp.float32) for m in members[key]], axis=0)

    stats = [stacked(key, slice(width, width + HD)) for key in range(SIDE)]
    peaks = [s + pltpu.roll(s, HD - 8, 1) + pltpu.roll(s, HD - 16, 1) for s in stats]
    sums = [pltpu.roll(s, HD - 24, 1) + pltpu.roll(s, HD - 32, 1) for s in stats]
    top = jnp.maximum(jnp.maximum(peaks[0], peaks[1]), jnp.maximum(peaks[2], peaks[3]))
    factors = [jnp.exp(p - top) for p in peaks]
    total = factors[0] * sums[0] + factors[1] * sums[1] + factors[2] * sums[2] + factors[3] * sums[3]
    lane = lax.broadcasted_iota(jnp.int32, total.shape, 1)
    inverse = 1.0 / jnp.where(lane < heads, total, 1.0)
    weights = [f * inverse for f in factors]
    for h in range(heads):
        acc = 0.0
        for key in range(SIDE):
            acc = acc + stacked(key, slice(h * HD, (h + 1) * HD)) * weights[key][:, h : h + 1]
        for g in range(SIDE):
            cols = slice(g * width + h * HD, g * width + (h + 1) * HD)
            rows = acc[g * 2 * half : (g + 1) * 2 * half].astype(jnp.bfloat16)
            image_out[:, cols] = rows[:half]
            text_out[:, cols] = rows[half:]


def local(
    image_query,
    image_key,
    image_value,
    text_query,
    text_key,
    text_value,
    image_query_gain,
    image_key_gain,
    text_query_gain,
    text_key_gain,
    image_order,
    text_length,
):
    rows, model = image_query.shape
    heads = model // HD
    width = model // SIDE
    text_rows = text_query.shape[0]
    block = text_rows // SIDE
    parts = SIDE * SIDE
    half = rows * SIDE**3 // 2
    bf, f32 = jnp.bfloat16, jnp.float32
    struct = jax.ShapeDtypeStruct
    gains = [g.reshape(1, HD) for g in (image_query_gain, image_key_gain, text_query_gain, text_key_gain)]

    own = vmem_call(
        lambda *refs: prep_kernel(heads, half, *refs),
        out_shape=[pltpu.VMEM((rows, 3 * width), bf)] * SIDE,
        in_specs=[HB] * 7,
        out_specs=[VM] * SIDE,
        scratch_shapes=[
            pltpu.SMEM((rows,), jnp.int32),
            pltpu.VMEM((1, HD), f32),
            pltpu.VMEM((rows, model), bf),
            pltpu.VMEM((rows, model), bf),
            pltpu.VMEM((rows, model), bf),
            pltpu.VMEM((1, HD), f32),
            pltpu.VMEM((1, HD), f32),
            pltpu.VMEM((rows, model), bf),
            pltpu.VMEM((rows, model), bf),
            pltpu.SemaphoreType.DMA((7,)),
        ],
        name="prep",
    )(image_order, jnp.asarray(frequencies()), image_query, image_key, image_value, gains[0], gains[1])

    from_y = [own[0]] + [exchange(own[d], HEAD_STEPS[d]) for d in range(1, SIDE)]

    qt, kt, vt, bias = vmem_call(
        text_kernel,
        out_shape=[pltpu.VMEM((block, width), bf)] * 3 + [pltpu.VMEM((8, block), f32)],
        in_specs=[HB] * 6,
        out_specs=[VM] * 4,
        scratch_shapes=[
            pltpu.SMEM((1,), jnp.int32),
            pltpu.VMEM((parts, block // parts, width), bf),
            pltpu.VMEM((block, width), bf),
            pltpu.VMEM((1, HD), f32),
            pltpu.VMEM((1, HD), f32),
            pltpu.SemaphoreType.DMA((5 + parts,)),
        ],
        cost_estimate=pl.CostEstimate(flops=20_000_000, bytes_accessed=600_000, transcendentals=0),
        name="text",
    )(text_query, text_key, text_value, gains[2], gains[3], text_length)

    kv, q = vmem_call(
        pack_kernel,
        out_shape=[pltpu.VMEM((SIDE * rows, 2 * width), bf), pltpu.VMEM((SIDE * rows, width), bf)],
        in_specs=[VM] * SIDE + [VM],
        out_specs=[VM] * 2,
        name="pack",
    )(*from_y, bias)

    q_next = exchange(q, QUERY_STEPS[1])
    kvs = [kv]
    for i in range(1, SIDE):
        kvs.append(exchange(kv, KEY_STEPS[i]))
    q_two = vmem_call(
        join_kernel,
        out_shape=pltpu.VMEM((2 * SIDE * rows, width), bf),
        in_specs=[VM] * 2,
        out_specs=VM,
        name="join",
    )(q, q_next)
    q_last = exchange(q_two, QUERY_STEPS[2])

    out_rows = rows + text_rows // SIDE**3
    partial = pl.pallas_call(
        attend_kernel,
        out_shape=pltpu.VMEM((parts, out_rows, width + HD), bf),
        in_specs=[VM] * 10,
        out_specs=VM,
        name="attend",
    )(*kvs, q_two, q_last, qt, kt, vt, bias)

    got = in_vmem(lax.all_to_all(partial, "seq", 0, 0, axis_index_groups=query_groups(), tiled=True))

    return pl.pallas_call(
        combine_kernel,
        out_shape=[struct((rows, model), bf), struct((out_rows - rows, model), bf)],
        in_specs=[VM],
        out_specs=[VM] * 2,
        name="combine",
    )(got)


def whole(*args):
    return tuple(local(*args))


def solution(mesh):
    token = P(("req", "seq"), None)
    text = P("req", None)
    return jax.shard_map(
        whole,
        mesh=mesh,
        in_specs=(token, token, token, text, text, text, P(), P(), P(), P(), P(("req", "seq")), P("req")),
        out_specs=(token, token),
        check_vma=False,
    )
```

```python
import jax
import jax.numpy as jnp
import numpy as np
from jax import lax
from jax.experimental import pallas as pl
from jax.experimental.pallas import tpu as pltpu
from jax.sharding import PartitionSpec as P

HD = 128
GRID_W = 64
SIDE = 4
EPS = 1e-06
MASKED = -1e30
SCALE = HD ** (-0.5)
LOG2E = 1.4426950408889634

VM = pl.BlockSpec(memory_space=pltpu.VMEM)
SM = pl.BlockSpec(memory_space=pltpu.SMEM)
HB = pl.BlockSpec(memory_space=pltpu.HBM)


ROLES = (1, 2, 0)


def split_index(i):
    raw = (i // (SIDE * SIDE), (i // SIDE) % SIDE, i % SIDE)
    return tuple(raw[r] for r in ROLES)


def join_index(x, z, y):
    raw = [None] * 3
    for r, c in zip(ROLES, (x, z, y)):
        raw[r] = c
    return (raw[0] * SIDE + raw[1]) * SIDE + raw[2]


def parity(i):
    return (i ^ (i >> 1)) & 1


def head_group(z, y):
    return parity(z) * 2 + parity(y)


def key_group(x, z):
    return parity(x) * 2 + (z >> 1)


def member(x, z, y):
    return parity(x) * 8 + z * 2 + (parity(y) ^ 1)


HEAD_STEPS = ((0, 0, 0), (0, 1, 1), (0, 1, 0), (0, 0, 1))
QUERY_STEPS = ((0, 0, 0), (0, 3, 0), (1, 0, 0), (1, 3, 0))
KEY_STEPS = ((0, 0, 0), (3, 0, 3), (3, 0, 0), (0, 0, 3))


def query_groups():
    groups = {}
    for i in range(SIDE**3):
        x, z, y = split_index(i)
        groups.setdefault((x >> 1, y >> 1), {})[member(x, z, y)] = i
    return [[g[j] for j in range(len(g))] for g in groups.values()]


def exchange(value, step):
    pairs = []
    for i in range(SIDE**3):
        x, z, y = split_index(i)
        pairs.append((i, join_index(x ^ step[0], z ^ step[1], y ^ step[2])))
    return in_vmem(lax.ppermute(value, "seq", pairs))


def in_vmem(value):
    return pltpu.with_memory_space_constraint(value, pltpu.VMEM)


def vmem_call(kernel, **options):
    call = pl.pallas_call(kernel, **options)
    return lambda *args: jax.tree.map(in_vmem, call(*args))


def head_norm(x, gain):
    mean_square = jnp.mean(x * x, axis=-1, keepdims=True)
    return x * lax.rsqrt(mean_square + EPS) * gain


def frequencies():
    pair = np.arange(HD) // 2
    within = np.where(pair < 8, pair, np.where(pair < 36, pair - 8, pair - 36)).astype(np.float64)
    dim = np.where(pair < 8, 16.0, 56.0)
    return (10000.0 ** (-2.0 * within / dim)).astype(np.float32).reshape(1, HD)


def load(pairs, sems):
    copies = [pltpu.make_async_copy(src, dst, sems.at[i]) for i, (src, dst) in enumerate(pairs)]
    for c in copies:
        c.start()
    for c in copies:
        c.wait()


def prep_kernel(heads, half, order_h, freq_h, q_h, k_h, v_h, qg_h, kg_h, o0, o1, o2, o3, order, freq, q_in, k_in, v_in, qg, kg, q_s, k_s, sems):
    load(
        ((order_h, order), (freq_h, freq), (q_h, q_in), (k_h, k_in), (v_h, v_in), (qg_h, qg), (kg_h, kg)),
        sems,
    )
    rows = q_in.shape[0]
    lane = lax.broadcasted_iota(jnp.int32, (rows, HD), 1)
    row = lax.broadcasted_iota(jnp.int32, (rows, HD), 0)
    position = jnp.zeros((rows, HD), jnp.int32)
    for i in range(rows):
        position = jnp.where(row == i, order[i], position)
    inside = position & (half - 1)
    pair = lane >> 1
    coordinate = jnp.where(
        pair < 8,
        position >> (half.bit_length() - 1),
        jnp.where(pair < 36, inside >> (GRID_W.bit_length() - 1), inside & (GRID_W - 1)),
    )
    angle = coordinate.astype(jnp.float32) * freq[...]
    cosine = jnp.cos(angle)
    sine = jnp.sin(angle)
    even = (lane & 1) == 0
    sine = jnp.where(even, -sine, sine)
    blocks = [
        src[:, h * HD : (h + 1) * HD].astype(jnp.float32) for src in (q_in, k_in) for h in range(heads)
    ]
    whole = jnp.concatenate(blocks, axis=0)
    mean_square = jnp.mean(whole * whole, axis=-1, keepdims=True)
    whole = whole * lax.rsqrt(mean_square + EPS)
    for n in range(2 * heads):
        gain, dst, h = (qg, q_s, n) if n < heads else (kg, k_s, n - heads)
        x = whole[n * rows : (n + 1) * rows] * gain[...]
        partner = jnp.where(even, pltpu.roll(x, HD - 1, 1), pltpu.roll(x, 1, 1))
        dst[:, h * HD : (h + 1) * HD] = (x * cosine + partner * sine).astype(jnp.bfloat16)
    width = heads // SIDE * HD
    _, z, y = split_index(lax.axis_index("seq"))
    for step, out in zip(HEAD_STEPS, (o0, o1, o2, o3)):
        start = pl.multiple_of(head_group(z ^ step[1], y ^ step[2]) * width, HD)
        out[:, 0:width] = k_s[:, pl.ds(start, width)]
        out[:, width : 2 * width] = v_in[:, pl.ds(start, width)]
        out[:, 2 * width : 3 * width] = q_s[:, pl.ds(start, width)]


def pack_kernel(a0, a1, a2, a3, order_only, kv, q):
    rows = a0.shape[0]
    width = q.shape[1]
    for j, a in enumerate((a0, a1, a2, a3)):
        kv[j * rows : (j + 1) * rows, :] = a[:, : 2 * width]
        q[j * rows : (j + 1) * rows, :] = a[:, 2 * width :]


def join_kernel(a, b, out):
    rows = a.shape[0]
    out[:rows, :] = a[...]
    out[rows:, :] = b[...]


def text_kernel(q_h, k_h, v_h, qg_h, kg_h, length_h, q_out, k_out, v_out, bias, length, q_in, k_in, qg, kg, sems):
    block, width = k_in.shape
    x, z, y = split_index(lax.axis_index("seq"))
    group = key_group(x, z)
    cols = pl.ds(pl.multiple_of(head_group(z, y) * width, HD), width)
    k_rows = pl.ds(pl.multiple_of(group * block, block), block)
    pieces = [
        (length_h, length),
        (k_h.at[k_rows, cols], k_in),
        (v_h.at[k_rows, cols], v_out),
        (qg_h, qg),
        (kg_h, kg),
    ]
    own = q_in.shape[1]
    for j in range(q_in.shape[0]):
        px, jz, py = j >> 3, (j >> 1) & 3, (j & 1) ^ 1
        jx = (x & 2) + (px ^ (x >> 1))
        jy = (y & 2) + (py ^ (y >> 1))
        start = join_index(jx, jz, jy) * own
        pieces.append((q_h.at[pl.ds(pl.multiple_of(start, own), own), cols], q_in.at[j]))
    load(pieces, sems)
    for gain, dst in ((qg, q_out), (kg, k_out)):
        g = gain[...]
        for h in range(width // HD):
            at = slice(h * HD, (h + 1) * HD)
            if dst is q_out:
                rows = q_in[:, :, at].astype(jnp.float32).reshape(block, HD)
            else:
                rows = k_in[:, at].astype(jnp.float32)
            dst[:, at] = head_norm(rows, g).astype(jnp.bfloat16)
    key = lax.broadcasted_iota(jnp.int32, bias.shape, 1) + group * block
    bias[...] = jnp.where(key < length[0], 0.0, MASKED)


def attend_kernel(kv0, kv1, kv2, kv3, q0, q1, qt, kt, vt, bias, out):
    kvs, qs = (kv0, kv1, kv2, kv3), (q0, q1)
    width = qt.shape[1]
    heads = width // HD
    text_keys = kt.shape[0]
    image_rows = 2 * q0.shape[0]
    rows = image_rows + qt.shape[0]
    x, z, y = split_index(lax.axis_index("seq"))
    masked = bias[0:1, :]
    lane = lax.broadcasted_iota(jnp.int32, (rows, HD), 1)
    stats = jnp.zeros((rows, HD), jnp.float32)
    blended = []
    for h in range(heads):
        cols = slice(h * HD, (h + 1) * HD)
        vcols = slice(width + h * HD, width + (h + 1) * HD)
        query = jnp.concatenate([r[:, cols] for r in qs] + [qt[:, cols]], axis=0)
        key = jnp.concatenate([kt[:, cols]] + [r[:, cols] for r in kvs], axis=0)
        value = jnp.concatenate([vt[:, cols]] + [r[:, vcols] for r in kvs], axis=0)
        s = lax.dot_general(query, key, (((1,), (1,)), ((), ())), preferred_element_type=jnp.float32)
        s = jnp.concatenate([s[:, :text_keys] + masked, s[:, text_keys:]], axis=1)
        m = jnp.max(s, axis=1, keepdims=True)
        e = jnp.exp2((s - m) * (SCALE * LOG2E))
        m = m * SCALE
        l = jnp.sum(e, axis=1, keepdims=True)
        blended.append(jnp.dot(e.astype(jnp.bfloat16), value, preferred_element_type=jnp.float32))
        for first, value in ((h, m), (24 + h, l)):
            for piece in range(3 if first == h else 2):
                stats = jnp.where(lane == first + 8 * piece, value, stats)
                value = value - value.astype(jnp.bfloat16).astype(jnp.float32)
    blended.append(stats)
    for a, key_step in enumerate(QUERY_STEPS):
        for b, head_step in enumerate(HEAD_STEPS):
            i = a * SIDE + b
            there = member(x ^ key_step[0], z ^ key_step[1] ^ head_step[1], y ^ head_step[2])
            for c, part in enumerate(blended):
                cols = slice(c * HD, (c + 1) * HD)
                out[there, 0:8, cols] = part[i * 8 : (i + 1) * 8].astype(jnp.bfloat16)
                begin = image_rows + i * 8
                out[i, 8:16, cols] = part[begin : begin + 8].astype(jnp.bfloat16)


def combine_kernel(got, image_out, text_out):
    heads = (got.shape[2] - HD) // HD
    width = heads * HD
    half = image_out.shape[0]
    members = [[None] * SIDE for _ in range(SIDE)]
    for j in range(got.shape[0]):
        px, z, py = j >> 3, (j >> 1) & 3, (j & 1) ^ 1
        members[px * 2 + (z >> 1)][parity(z) * 2 + py] = j

    def stacked(key, cols):
        return jnp.concatenate([got[m, :, cols].astype(jnp.float32) for m in members[key]], axis=0)

    stats = [stacked(key, slice(width, width + HD)) for key in range(SIDE)]
    peaks = [s + pltpu.roll(s, HD - 8, 1) + pltpu.roll(s, HD - 16, 1) for s in stats]
    sums = [pltpu.roll(s, HD - 24, 1) + pltpu.roll(s, HD - 32, 1) for s in stats]
    top = jnp.maximum(jnp.maximum(peaks[0], peaks[1]), jnp.maximum(peaks[2], peaks[3]))
    factors = [jnp.exp(p - top) for p in peaks]
    total = factors[0] * sums[0] + factors[1] * sums[1] + factors[2] * sums[2] + factors[3] * sums[3]
    lane = lax.broadcasted_iota(jnp.int32, total.shape, 1)
    inverse = 1.0 / jnp.where(lane < heads, total, 1.0)
    weights = [f * inverse for f in factors]
    for h in range(heads):
        acc = 0.0
        for key in range(SIDE):
            acc = acc + stacked(key, slice(h * HD, (h + 1) * HD)) * weights[key][:, h : h + 1]
        for g in range(SIDE):
            cols = slice(g * width + h * HD, g * width + (h + 1) * HD)
            rows = acc[g * 2 * half : (g + 1) * 2 * half].astype(jnp.bfloat16)
            image_out[:, cols] = rows[:half]
            text_out[:, cols] = rows[half:]


def local(
    image_query,
    image_key,
    image_value,
    text_query,
    text_key,
    text_value,
    image_query_gain,
    image_key_gain,
    text_query_gain,
    text_key_gain,
    image_order,
    text_length,
):
    rows, model = image_query.shape
    heads = model // HD
    width = model // SIDE
    text_rows = text_query.shape[0]
    block = text_rows // SIDE
    parts = SIDE * SIDE
    half = rows * SIDE**3 // 2
    bf, f32 = jnp.bfloat16, jnp.float32
    struct = jax.ShapeDtypeStruct
    gains = [g.reshape(1, HD) for g in (image_query_gain, image_key_gain, text_query_gain, text_key_gain)]

    own = vmem_call(
        lambda *refs: prep_kernel(heads, half, *refs),
        out_shape=[pltpu.VMEM((rows, 3 * width), bf)] * SIDE,
        in_specs=[HB] * 7,
        out_specs=[VM] * SIDE,
        scratch_shapes=[
            pltpu.SMEM((rows,), jnp.int32),
            pltpu.VMEM((1, HD), f32),
            pltpu.VMEM((rows, model), bf),
            pltpu.VMEM((rows, model), bf),
            pltpu.VMEM((rows, model), bf),
            pltpu.VMEM((1, HD), f32),
            pltpu.VMEM((1, HD), f32),
            pltpu.VMEM((rows, model), bf),
            pltpu.VMEM((rows, model), bf),
            pltpu.SemaphoreType.DMA((7,)),
        ],
        name="prep",
    )(image_order, jnp.asarray(frequencies()), image_query, image_key, image_value, gains[0], gains[1])

    from_y = [own[0]] + [exchange(own[d], HEAD_STEPS[d]) for d in range(1, SIDE)]

    qt, kt, vt, bias = vmem_call(
        text_kernel,
        out_shape=[pltpu.VMEM((block, width), bf)] * 3 + [pltpu.VMEM((8, block), f32)],
        in_specs=[HB] * 6,
        out_specs=[VM] * 4,
        scratch_shapes=[
            pltpu.SMEM((1,), jnp.int32),
            pltpu.VMEM((parts, block // parts, width), bf),
            pltpu.VMEM((block, width), bf),
            pltpu.VMEM((1, HD), f32),
            pltpu.VMEM((1, HD), f32),
            pltpu.SemaphoreType.DMA((5 + parts,)),
        ],
        cost_estimate=pl.CostEstimate(flops=20_000_000, bytes_accessed=600_000, transcendentals=0),
        name="text",
    )(text_query, text_key, text_value, gains[2], gains[3], text_length)

    kv, q = vmem_call(
        pack_kernel,
        out_shape=[pltpu.VMEM((SIDE * rows, 2 * width), bf), pltpu.VMEM((SIDE * rows, width), bf)],
        in_specs=[VM] * SIDE + [VM],
        out_specs=[VM] * 2,
        name="pack",
    )(*from_y, bias)

    q_next = exchange(q, QUERY_STEPS[1])
    kvs = [kv]
    for i in range(1, SIDE):
        kvs.append(exchange(kv, KEY_STEPS[i]))
    q_two = vmem_call(
        join_kernel,
        out_shape=pltpu.VMEM((2 * SIDE * rows, width), bf),
        in_specs=[VM] * 2,
        out_specs=VM,
        name="join",
    )(q, q_next)
    q_last = exchange(q_two, QUERY_STEPS[2])

    out_rows = rows + text_rows // SIDE**3
    partial = pl.pallas_call(
        attend_kernel,
        out_shape=pltpu.VMEM((parts, out_rows, width + HD), bf),
        in_specs=[VM] * 10,
        out_specs=VM,
        name="attend",
    )(*kvs, q_two, q_last, qt, kt, vt, bias)

    got = in_vmem(lax.all_to_all(partial, "seq", 0, 0, axis_index_groups=query_groups(), tiled=True))

    return pl.pallas_call(
        combine_kernel,
        out_shape=[struct((rows, model), bf), struct((out_rows - rows, model), bf)],
        in_specs=[VM],
        out_specs=[VM] * 2,
        name="combine",
    )(got)


def whole(*args):
    return tuple(local(*args))


def solution(mesh):
    token = P(("req", "seq"), None)
    text = P("req", None)
    return jax.shard_map(
        whole,
        mesh=mesh,
        in_specs=(token, token, token, text, text, text, P(), P(), P(), P(), P(("req", "seq")), P("req")),
        out_specs=(token, token),
        check_vma=False,
    )
```

```python
import jax
import jax.numpy as jnp
import numpy as np
from jax import lax
from jax.experimental import pallas as pl
from jax.experimental.pallas import tpu as pltpu
from jax.sharding import PartitionSpec as P

HD = 128
GRID_W = 64
SIDE = 4
EPS = 1e-06
MASKED = -1e30
SCALE = HD ** (-0.5)
LOG2E = 1.4426950408889634

VM = pl.BlockSpec(memory_space=pltpu.VMEM)
SM = pl.BlockSpec(memory_space=pltpu.SMEM)
HB = pl.BlockSpec(memory_space=pltpu.HBM)


ROLES = (1, 2, 0)


def split_index(i):
    raw = (i // (SIDE * SIDE), (i // SIDE) % SIDE, i % SIDE)
    return tuple(raw[r] for r in ROLES)


def join_index(x, z, y):
    raw = [None] * 3
    for r, c in zip(ROLES, (x, z, y)):
        raw[r] = c
    return (raw[0] * SIDE + raw[1]) * SIDE + raw[2]


def parity(i):
    return (i ^ (i >> 1)) & 1


def head_group(z, y):
    return parity(z) * 2 + parity(y)


def key_group(x, z):
    return parity(x) * 2 + (z >> 1)


def member(x, z, y):
    return parity(x) * 8 + z * 2 + (parity(y) ^ 1)


HEAD_STEPS = ((0, 0, 0), (0, 1, 1), (0, 1, 0), (0, 0, 1))
QUERY_STEPS = ((0, 0, 0), (0, 3, 0), (1, 0, 0), (1, 3, 0))
KEY_STEPS = ((0, 0, 0), (3, 0, 3), (3, 0, 0), (0, 0, 3))


def query_groups():
    groups = {}
    for i in range(SIDE**3):
        x, z, y = split_index(i)
        groups.setdefault((x >> 1, y >> 1), {})[member(x, z, y)] = i
    return [[g[j] for j in range(len(g))] for g in groups.values()]


def exchange(value, step):
    pairs = []
    for i in range(SIDE**3):
        x, z, y = split_index(i)
        pairs.append((i, join_index(x ^ step[0], z ^ step[1], y ^ step[2])))
    return in_vmem(lax.ppermute(value, "seq", pairs))


def in_vmem(value):
    return pltpu.with_memory_space_constraint(value, pltpu.VMEM)


def vmem_call(kernel, **options):
    call = pl.pallas_call(kernel, **options)
    return lambda *args: jax.tree.map(in_vmem, call(*args))


def head_norm(x, gain):
    mean_square = jnp.mean(x * x, axis=-1, keepdims=True)
    return x * lax.rsqrt(mean_square + EPS) * gain


def frequencies():
    pair = np.arange(HD) // 2
    within = np.where(pair < 8, pair, np.where(pair < 36, pair - 8, pair - 36)).astype(np.float64)
    dim = np.where(pair < 8, 16.0, 56.0)
    return (10000.0 ** (-2.0 * within / dim)).astype(np.float32).reshape(1, HD)


def load(pairs, sems):
    copies = [pltpu.make_async_copy(src, dst, sems.at[i]) for i, (src, dst) in enumerate(pairs)]
    for c in copies:
        c.start()
    for c in copies:
        c.wait()


def prep_kernel(heads, half, order_h, freq_h, q_h, k_h, v_h, qg_h, kg_h, o0, o1, o2, o3, order, freq, q_in, k_in, v_in, qg, kg, q_s, k_s, sems):
    load(
        ((order_h, order), (freq_h, freq), (q_h, q_in), (k_h, k_in), (v_h, v_in), (qg_h, qg), (kg_h, kg)),
        sems,
    )
    rows = q_in.shape[0]
    lane = lax.broadcasted_iota(jnp.int32, (rows, HD), 1)
    row = lax.broadcasted_iota(jnp.int32, (rows, HD), 0)
    position = jnp.zeros((rows, HD), jnp.int32)
    for i in range(rows):
        position = jnp.where(row == i, order[i], position)
    inside = position & (half - 1)
    pair = lane >> 1
    coordinate = jnp.where(
        pair < 8,
        position >> (half.bit_length() - 1),
        jnp.where(pair < 36, inside >> (GRID_W.bit_length() - 1), inside & (GRID_W - 1)),
    )
    angle = coordinate.astype(jnp.float32) * freq[...]
    cosine = jnp.cos(angle)
    sine = jnp.sin(angle)
    even = (lane & 1) == 0
    sine = jnp.where(even, -sine, sine)
    blocks = [
        src[:, h * HD : (h + 1) * HD].astype(jnp.float32) for src in (q_in, k_in) for h in range(heads)
    ]
    whole = jnp.concatenate(blocks, axis=0)
    mean_square = jnp.mean(whole * whole, axis=-1, keepdims=True)
    whole = whole * lax.rsqrt(mean_square + EPS)
    for n in range(2 * heads):
        gain, dst, h = (qg, q_s, n) if n < heads else (kg, k_s, n - heads)
        x = whole[n * rows : (n + 1) * rows] * gain[...]
        partner = jnp.where(even, pltpu.roll(x, HD - 1, 1), pltpu.roll(x, 1, 1))
        dst[:, h * HD : (h + 1) * HD] = (x * cosine + partner * sine).astype(jnp.bfloat16)
    width = heads // SIDE * HD
    _, z, y = split_index(lax.axis_index("seq"))
    for step, out in zip(HEAD_STEPS, (o0, o1, o2, o3)):
        start = pl.multiple_of(head_group(z ^ step[1], y ^ step[2]) * width, HD)
        out[:, 0:width] = k_s[:, pl.ds(start, width)]
        out[:, width : 2 * width] = v_in[:, pl.ds(start, width)]
        out[:, 2 * width : 3 * width] = q_s[:, pl.ds(start, width)]


def pack_kernel(a0, a1, a2, a3, order_only, kv, q):
    rows = a0.shape[0]
    width = q.shape[1]
    for j, a in enumerate((a0, a1, a2, a3)):
        kv[j * rows : (j + 1) * rows, :] = a[:, : 2 * width]
        q[j * rows : (j + 1) * rows, :] = a[:, 2 * width :]


def join_kernel(a, b, out):
    rows = a.shape[0]
    out[:rows, :] = a[...]
    out[rows:, :] = b[...]


def text_kernel(q_h, k_h, v_h, qg_h, kg_h, length_h, q_out, k_out, v_out, bias, length, q_in, k_in, qg, kg, sems):
    block, width = k_in.shape
    x, z, y = split_index(lax.axis_index("seq"))
    group = key_group(x, z)
    cols = pl.ds(pl.multiple_of(head_group(z, y) * width, HD), width)
    k_rows = pl.ds(pl.multiple_of(group * block, block), block)
    pieces = [
        (length_h, length),
        (k_h.at[k_rows, cols], k_in),
        (v_h.at[k_rows, cols], v_out),
        (qg_h, qg),
        (kg_h, kg),
    ]
    own = q_in.shape[1]
    for j in range(q_in.shape[0]):
        px, jz, py = j >> 3, (j >> 1) & 3, (j & 1) ^ 1
        jx = (x & 2) + (px ^ (x >> 1))
        jy = (y & 2) + (py ^ (y >> 1))
        start = join_index(jx, jz, jy) * own
        pieces.append((q_h.at[pl.ds(pl.multiple_of(start, own), own), cols], q_in.at[j]))
    load(pieces, sems)
    for gain, dst in ((qg, q_out), (kg, k_out)):
        g = gain[...]
        for h in range(width // HD):
            at = slice(h * HD, (h + 1) * HD)
            if dst is q_out:
                rows = q_in[:, :, at].astype(jnp.float32).reshape(block, HD)
            else:
                rows = k_in[:, at].astype(jnp.float32)
            dst[:, at] = head_norm(rows, g).astype(jnp.bfloat16)
    key = lax.broadcasted_iota(jnp.int32, bias.shape, 1) + group * block
    bias[...] = jnp.where(key < length[0], 0.0, MASKED)


def attend(queries, kvs, kt, vt, bias, base):
    width = kt.shape[1]
    text_keys = kt.shape[0]
    masked = bias[0:1, :]
    rows = sum(r.shape[0] for r in queries)
    lane = lax.broadcasted_iota(jnp.int32, (rows, HD), 1) - base
    stats = jnp.zeros((rows, HD), jnp.float32)
    blended = []
    for h in range(width // HD):
        cols = slice(h * HD, (h + 1) * HD)
        vcols = slice(width + h * HD, width + (h + 1) * HD)
        query = jnp.concatenate([r[:, cols] for r in queries], axis=0)
        key = jnp.concatenate([kt[:, cols]] + [r[:, cols] for r in kvs], axis=0)
        value = jnp.concatenate([vt[:, cols]] + [r[:, vcols] for r in kvs], axis=0)
        s = lax.dot_general(query, key, (((1,), (1,)), ((), ())), preferred_element_type=jnp.float32)
        s = jnp.concatenate([s[:, :text_keys] + masked, s[:, text_keys:]], axis=1)
        m = jnp.max(s, axis=1, keepdims=True)
        e = jnp.exp2((s - m) * (SCALE * LOG2E))
        m = m * SCALE
        l = jnp.sum(e, axis=1, keepdims=True)
        blended.append(jnp.dot(e.astype(jnp.bfloat16), value, preferred_element_type=jnp.float32))
        for first, value, pieces in ((h, m, 3), (24 + h, l, 2)):
            for piece in range(pieces):
                stats = jnp.where(lane == first + 8 * piece, value, stats)
                value = value - value.astype(jnp.bfloat16).astype(jnp.float32)
    return blended + [stats]


def attend_kernel(kv0, kv1, kv2, kv3, q0, q1, qt, kt, vt, bias, out):
    kvs = (kv0, kv1, kv2, kv3)
    half = HD // 2
    heads = qt.shape[1] // HD
    x, z, y = split_index(lax.axis_index("seq"))
    text = attend((qt,), kvs, kt, vt, bias, half)
    for j in range(out.shape[0]):
        for c, part in enumerate(text):
            rows = part[j * 8 : (j + 1) * 8].astype(jnp.bfloat16)
            if c < heads:
                out[j, :, (heads + c) * HD : (heads + c + 1) * HD] = rows
            else:
                out[j, :, 2 * heads * HD + half :] = rows[:, half:]
    image = attend((q0, q1), kvs, kt, vt, bias, 0)
    for a, key_step in enumerate(QUERY_STEPS):
        for b, head_step in enumerate(HEAD_STEPS):
            i = a * SIDE + b
            there = member(x ^ key_step[0], z ^ key_step[1] ^ head_step[1], y ^ head_step[2])
            for c, part in enumerate(image):
                rows = part[i * 8 : (i + 1) * 8].astype(jnp.bfloat16)
                if c < heads:
                    out[there, :, c * HD : (c + 1) * HD] = rows
                else:
                    out[there, :, 2 * heads * HD : 2 * heads * HD + half] = rows[:, :half]


def combine_kernel(got, image_out, text_out, image_s, text_s, sems):
    heads = (got.shape[2] - HD) // HD // 2
    width = heads * HD
    rows = got.shape[1]
    members = [[None] * SIDE for _ in range(SIDE)]
    for j in range(got.shape[0]):
        px, z, py = j >> 3, (j >> 1) & 3, (j & 1) ^ 1
        members[px * 2 + (z >> 1)][parity(z) * 2 + py] = j

    def stacked(key, block):
        cols = slice(block * HD, (block + 1) * HD)
        return jnp.concatenate([got[m, :, cols].astype(jnp.float32) for m in members[key]], axis=0)

    stats = [stacked(key, 2 * heads) for key in range(SIDE)]
    peaks = [s + pltpu.roll(s, HD - 8, 1) + pltpu.roll(s, HD - 16, 1) for s in stats]
    sums = [pltpu.roll(s, HD - 24, 1) + pltpu.roll(s, HD - 32, 1) for s in stats]
    top = jnp.maximum(jnp.maximum(peaks[0], peaks[1]), jnp.maximum(peaks[2], peaks[3]))
    factors = [jnp.exp(p - top) for p in peaks]
    total = factors[0] * sums[0] + factors[1] * sums[1] + factors[2] * sums[2] + factors[3] * sums[3]
    lane = lax.broadcasted_iota(jnp.int32, total.shape, 1) & (HD // 2 - 1)
    inverse = 1.0 / jnp.where(lane < heads, total, 1.0)
    weights = [f * inverse for f in factors]
    copies = []
    for t, (dst, scratch) in enumerate(((image_out, image_s), (text_out, text_s))):
        for h in range(heads):
            at = t * (HD // 2) + h
            acc = 0.0
            for key in range(SIDE):
                acc = acc + stacked(key, t * heads + h) * weights[key][:, at : at + 1]
            for g in range(SIDE):
                cols = slice(g * width + h * HD, g * width + (h + 1) * HD)
                scratch[:, cols] = acc[g * rows : (g + 1) * rows].astype(jnp.bfloat16)
        copies.append(pltpu.make_async_copy(scratch, dst, sems.at[t]))
        copies[-1].start()
    for c in copies:
        c.wait()


def local(
    image_query,
    image_key,
    image_value,
    text_query,
    text_key,
    text_value,
    image_query_gain,
    image_key_gain,
    text_query_gain,
    text_key_gain,
    image_order,
    text_length,
):
    rows, model = image_query.shape
    heads = model // HD
    width = model // SIDE
    text_rows = text_query.shape[0]
    block = text_rows // SIDE
    parts = SIDE * SIDE
    half = rows * SIDE**3 // 2
    bf, f32 = jnp.bfloat16, jnp.float32
    struct = jax.ShapeDtypeStruct
    gains = [g.reshape(1, HD) for g in (image_query_gain, image_key_gain, text_query_gain, text_key_gain)]

    own = vmem_call(
        lambda *refs: prep_kernel(heads, half, *refs),
        out_shape=[pltpu.VMEM((rows, 3 * width), bf)] * SIDE,
        in_specs=[HB] * 7,
        out_specs=[VM] * SIDE,
        scratch_shapes=[
            pltpu.SMEM((rows,), jnp.int32),
            pltpu.VMEM((1, HD), f32),
            pltpu.VMEM((rows, model), bf),
            pltpu.VMEM((rows, model), bf),
            pltpu.VMEM((rows, model), bf),
            pltpu.VMEM((1, HD), f32),
            pltpu.VMEM((1, HD), f32),
            pltpu.VMEM((rows, model), bf),
            pltpu.VMEM((rows, model), bf),
            pltpu.SemaphoreType.DMA((7,)),
        ],
        name="prep",
    )(image_order, jnp.asarray(frequencies()), image_query, image_key, image_value, gains[0], gains[1])

    from_y = [own[0]] + [exchange(own[d], HEAD_STEPS[d]) for d in range(1, SIDE)]

    qt, kt, vt, bias = vmem_call(
        text_kernel,
        out_shape=[pltpu.VMEM((block, width), bf)] * 3 + [pltpu.VMEM((8, block), f32)],
        in_specs=[HB] * 6,
        out_specs=[VM] * 4,
        scratch_shapes=[
            pltpu.SMEM((1,), jnp.int32),
            pltpu.VMEM((parts, block // parts, width), bf),
            pltpu.VMEM((block, width), bf),
            pltpu.VMEM((1, HD), f32),
            pltpu.VMEM((1, HD), f32),
            pltpu.SemaphoreType.DMA((5 + parts,)),
        ],
        cost_estimate=pl.CostEstimate(flops=20_000_000, bytes_accessed=600_000, transcendentals=0),
        name="text",
    )(text_query, text_key, text_value, gains[2], gains[3], text_length)

    kv, q = vmem_call(
        pack_kernel,
        out_shape=[pltpu.VMEM((SIDE * rows, 2 * width), bf), pltpu.VMEM((SIDE * rows, width), bf)],
        in_specs=[VM] * SIDE + [VM],
        out_specs=[VM] * 2,
        name="pack",
    )(*from_y, bias)

    q_next = exchange(q, QUERY_STEPS[1])
    kvs = [kv]
    for i in range(1, SIDE):
        kvs.append(exchange(kv, KEY_STEPS[i]))
    q_two = vmem_call(
        join_kernel,
        out_shape=pltpu.VMEM((2 * SIDE * rows, width), bf),
        in_specs=[VM] * 2,
        out_specs=VM,
        name="join",
    )(q, q_next)
    q_last = exchange(q_two, QUERY_STEPS[2])

    partial = pl.pallas_call(
        attend_kernel,
        out_shape=pltpu.VMEM((parts, rows, 2 * width + HD), bf),
        in_specs=[VM] * 10,
        out_specs=VM,
        name="attend",
    )(*kvs, q_two, q_last, qt, kt, vt, bias)

    got = in_vmem(lax.all_to_all(partial, "seq", 0, 0, axis_index_groups=query_groups(), tiled=True))

    own_text = text_rows // SIDE**3
    return pl.pallas_call(
        combine_kernel,
        out_shape=[struct((rows, model), bf), struct((own_text, model), bf)],
        in_specs=[VM],
        out_specs=[HB] * 2,
        scratch_shapes=[
            pltpu.VMEM((rows, model), bf),
            pltpu.VMEM((own_text, model), bf),
            pltpu.SemaphoreType.DMA((2,)),
        ],
        name="combine",
    )(got)


def whole(*args):
    return tuple(local(*args))


def solution(mesh):
    token = P(("req", "seq"), None)
    text = P("req", None)
    return jax.shard_map(
        whole,
        mesh=mesh,
        in_specs=(token, token, token, text, text, text, P(), P(), P(), P(), P(("req", "seq")), P("req")),
        out_specs=(token, token),
        check_vma=False,
    )
```

```python
import jax
import jax.numpy as jnp
import numpy as np
from jax import lax
from jax.experimental import pallas as pl
from jax.experimental.pallas import tpu as pltpu
from jax.sharding import PartitionSpec as P

HD = 128
GRID_W = 64
SIDE = 4
EPS = 1e-06
MASKED = -1e30
SCALE = HD ** (-0.5)
LOG2E = 1.4426950408889634

VM = pl.BlockSpec(memory_space=pltpu.VMEM)
SM = pl.BlockSpec(memory_space=pltpu.SMEM)
HB = pl.BlockSpec(memory_space=pltpu.HBM)


ROLES = (1, 2, 0)


def split_index(i):
    raw = (i // (SIDE * SIDE), (i // SIDE) % SIDE, i % SIDE)
    return tuple(raw[r] for r in ROLES)


def join_index(x, z, y):
    raw = [None] * 3
    for r, c in zip(ROLES, (x, z, y)):
        raw[r] = c
    return (raw[0] * SIDE + raw[1]) * SIDE + raw[2]


def parity(i):
    return (i ^ (i >> 1)) & 1


def head_group(z, y):
    return parity(z) * 2 + parity(y)


def key_group(x, z):
    return parity(x) * 2 + (z >> 1)


def member(x, z, y):
    return parity(x) * 8 + z * 2 + (parity(y) ^ 1)


HEAD_STEPS = ((0, 0, 0), (0, 1, 0), (0, 1, 1), (0, 0, 1))
QUERY_STEPS = ((0, 0, 0), (0, 3, 0), (1, 0, 0), (1, 3, 0))
KEY_STEPS = ((0, 0, 0), (3, 0, 3), (3, 0, 0), (0, 0, 3))


def query_groups():
    groups = {}
    for i in range(SIDE**3):
        x, z, y = split_index(i)
        groups.setdefault((x >> 1, y >> 1), {})[member(x, z, y)] = i
    return [[g[j] for j in range(len(g))] for g in groups.values()]


def exchange(value, step):
    pairs = []
    for i in range(SIDE**3):
        x, z, y = split_index(i)
        pairs.append((i, join_index(x ^ step[0], z ^ step[1], y ^ step[2])))
    return in_vmem(lax.ppermute(value, "seq", pairs))


def in_vmem(value):
    return pltpu.with_memory_space_constraint(value, pltpu.VMEM)


def vmem_call(kernel, **options):
    call = pl.pallas_call(kernel, **options)
    return lambda *args: jax.tree.map(in_vmem, call(*args))


def head_norm(x, gain):
    mean_square = jnp.mean(x * x, axis=-1, keepdims=True)
    return x * lax.rsqrt(mean_square + EPS) * gain


def frequencies():
    pair = np.arange(HD) // 2
    within = np.where(pair < 8, pair, np.where(pair < 36, pair - 8, pair - 36)).astype(np.float64)
    dim = np.where(pair < 8, 16.0, 56.0)
    return (10000.0 ** (-2.0 * within / dim)).astype(np.float32).reshape(1, HD)


def load(pairs, sems):
    copies = [pltpu.make_async_copy(src, dst, sems.at[i]) for i, (src, dst) in enumerate(pairs)]
    for c in copies:
        c.start()
    for c in copies:
        c.wait()


def prep_kernel(heads, half, order_h, freq_h, q_h, k_h, v_h, qg_h, kg_h, o0, o1, o2, o3, order, freq, q_in, k_in, v_in, qg, kg, q_s, k_s, sems):
    load(
        ((order_h, order), (freq_h, freq), (q_h, q_in), (k_h, k_in), (v_h, v_in), (qg_h, qg), (kg_h, kg)),
        sems,
    )
    rows = q_in.shape[0]
    lane = lax.broadcasted_iota(jnp.int32, (rows, HD), 1)
    row = lax.broadcasted_iota(jnp.int32, (rows, HD), 0)
    position = jnp.zeros((rows, HD), jnp.int32)
    for i in range(rows):
        position = jnp.where(row == i, order[i], position)
    inside = position & (half - 1)
    pair = lane >> 1
    coordinate = jnp.where(
        pair < 8,
        position >> (half.bit_length() - 1),
        jnp.where(pair < 36, inside >> (GRID_W.bit_length() - 1), inside & (GRID_W - 1)),
    )
    angle = coordinate.astype(jnp.float32) * freq[...]
    cosine = jnp.cos(angle)
    sine = jnp.sin(angle)
    even = (lane & 1) == 0
    sine = jnp.where(even, -sine, sine)
    blocks = [
        src[:, h * HD : (h + 1) * HD].astype(jnp.float32) for src in (q_in, k_in) for h in range(heads)
    ]
    whole = jnp.concatenate(blocks, axis=0)
    mean_square = jnp.mean(whole * whole, axis=-1, keepdims=True)
    whole = whole * lax.rsqrt(mean_square + EPS)
    for n in range(2 * heads):
        gain, dst, h = (qg, q_s, n) if n < heads else (kg, k_s, n - heads)
        x = whole[n * rows : (n + 1) * rows] * gain[...]
        partner = jnp.where(even, pltpu.roll(x, HD - 1, 1), pltpu.roll(x, 1, 1))
        dst[:, h * HD : (h + 1) * HD] = (x * cosine + partner * sine).astype(jnp.bfloat16)
    width = heads // SIDE * HD
    _, z, y = split_index(lax.axis_index("seq"))
    for step, out in zip(HEAD_STEPS, (o0, o1, o2, o3)):
        start = pl.multiple_of(head_group(z ^ step[1], y ^ step[2]) * width, HD)
        out[:, 0:width] = k_s[:, pl.ds(start, width)]
        out[:, width : 2 * width] = v_in[:, pl.ds(start, width)]
        out[:, 2 * width : 3 * width] = q_s[:, pl.ds(start, width)]


def pack_kernel(a0, a1, a2, a3, kv, q):
    rows = a0.shape[0]
    width = q.shape[1]
    for j, a in enumerate((a0, a1, a2, a3)):
        kv[j * rows : (j + 1) * rows, :] = a[:, : 2 * width]
        q[j * rows : (j + 1) * rows, :] = a[:, 2 * width :]


def join_kernel(a, b, out):
    rows = a.shape[0]
    out[:rows, :] = a[...]
    out[rows:, :] = b[...]


def text_kernel(q_h, k_h, v_h, qg_h, kg_h, length_h, q_out, k_out, v_out, bias, length, q_in, k_in, qg, kg, sems):
    block, width = k_in.shape
    x, z, y = split_index(lax.axis_index("seq"))
    group = key_group(x, z)
    cols = pl.ds(pl.multiple_of(head_group(z, y) * width, HD), width)
    k_rows = pl.ds(pl.multiple_of(group * block, block), block)
    pieces = [
        (length_h, length),
        (k_h.at[k_rows, cols], k_in),
        (v_h.at[k_rows, cols], v_out),
        (qg_h, qg),
        (kg_h, kg),
    ]
    own = q_in.shape[1]
    for j in range(q_in.shape[0]):
        px, jz, py = j >> 3, (j >> 1) & 3, (j & 1) ^ 1
        jx = (x & 2) + (px ^ (x >> 1))
        jy = (y & 2) + (py ^ (y >> 1))
        start = join_index(jx, jz, jy) * own
        pieces.append((q_h.at[pl.ds(pl.multiple_of(start, own), own), cols], q_in.at[j]))
    load(pieces, sems)
    for gain, dst in ((qg, q_out), (kg, k_out)):
        g = gain[...]
        for h in range(width // HD):
            at = slice(h * HD, (h + 1) * HD)
            if dst is q_out:
                rows = q_in[:, :, at].astype(jnp.float32).reshape(block, HD)
            else:
                rows = k_in[:, at].astype(jnp.float32)
            dst[:, at] = head_norm(rows, g).astype(jnp.bfloat16)
    key = lax.broadcasted_iota(jnp.int32, bias.shape, 1) + group * block
    bias[...] = jnp.where(key < length[0], 0.0, MASKED)


def attend(queries, kvs, kt, vt, bias, base):
    width = kt.shape[1]
    text_keys = kt.shape[0]
    masked = bias[0:1, :]
    rows = sum(r.shape[0] for r in queries)
    lane = lax.broadcasted_iota(jnp.int32, (rows, HD), 1) - base
    stats = jnp.zeros((rows, HD), jnp.float32)
    heads = range(width // HD)
    scores = []
    for h in heads:
        cols = slice(h * HD, (h + 1) * HD)
        query = jnp.concatenate([r[:, cols] for r in queries], axis=0)
        key = jnp.concatenate([kt[:, cols]] + [r[:, cols] for r in kvs], axis=0)
        s = lax.dot_general(query, key, (((1,), (1,)), ((), ())), preferred_element_type=jnp.float32)
        scores.append(jnp.concatenate([s[:, :text_keys] + masked, s[:, text_keys:]], axis=1))
    tops = [jnp.max(s, axis=1, keepdims=True) for s in scores]
    weights = [jnp.exp2((s - m) * (SCALE * LOG2E)) for s, m in zip(scores, tops)]
    blended = []
    for h in heads:
        cols = slice(h * HD, (h + 1) * HD)
        vcols = slice(width + h * HD, width + (h + 1) * HD)
        value = jnp.concatenate([vt[:, cols]] + [r[:, vcols] for r in kvs], axis=0)
        blended.append(jnp.dot(weights[h].astype(jnp.bfloat16), value, preferred_element_type=jnp.float32))
    totals = [jnp.sum(e, axis=1, keepdims=True) for e in weights]
    for h in heads:
        for first, value, pieces in ((h, tops[h] * SCALE, 3), (24 + h, totals[h], 2)):
            for piece in range(pieces):
                stats = jnp.where(lane == first + 8 * piece, value, stats)
                value = value - value.astype(jnp.bfloat16).astype(jnp.float32)
    return blended + [stats]


def attend_kernel(kv0, kv1, kv2, kv3, q0, q1, qt, kt, vt, bias, out):
    kvs = (kv0, kv1, kv2, kv3)
    half = HD // 2
    heads = qt.shape[1] // HD
    x, z, y = split_index(lax.axis_index("seq"))
    text = attend((qt,), kvs, kt, vt, bias, half)
    for j in range(out.shape[0]):
        for c, part in enumerate(text):
            rows = part[j * 8 : (j + 1) * 8].astype(jnp.bfloat16)
            if c < heads:
                out[j, :, (heads + c) * HD : (heads + c + 1) * HD] = rows
            else:
                out[j, :, 2 * heads * HD + half :] = rows[:, half:]
    image = attend((q0, q1), kvs, kt, vt, bias, 0)
    for a, key_step in enumerate(QUERY_STEPS):
        for b, head_step in enumerate(HEAD_STEPS):
            i = a * SIDE + b
            there = member(x ^ key_step[0], z ^ key_step[1] ^ head_step[1], y ^ head_step[2])
            for c, part in enumerate(image):
                rows = part[i * 8 : (i + 1) * 8].astype(jnp.bfloat16)
                if c < heads:
                    out[there, :, c * HD : (c + 1) * HD] = rows
                else:
                    out[there, :, 2 * heads * HD : 2 * heads * HD + half] = rows[:, :half]


def combine_kernel(got, image_out, text_out, image_s, text_s, sems):
    heads = (got.shape[2] - HD) // HD // 2
    width = heads * HD
    rows = got.shape[1]
    members = [[None] * SIDE for _ in range(SIDE)]
    for j in range(got.shape[0]):
        px, z, py = j >> 3, (j >> 1) & 3, (j & 1) ^ 1
        members[px * 2 + (z >> 1)][parity(z) * 2 + py] = j

    def stacked(key, block):
        cols = slice(block * HD, (block + 1) * HD)
        return jnp.concatenate([got[m, :, cols].astype(jnp.float32) for m in members[key]], axis=0)

    stats = [stacked(key, 2 * heads) for key in range(SIDE)]
    peaks = [s + pltpu.roll(s, HD - 8, 1) + pltpu.roll(s, HD - 16, 1) for s in stats]
    sums = [pltpu.roll(s, HD - 24, 1) + pltpu.roll(s, HD - 32, 1) for s in stats]
    top = jnp.maximum(jnp.maximum(peaks[0], peaks[1]), jnp.maximum(peaks[2], peaks[3]))
    factors = [jnp.exp(p - top) for p in peaks]
    total = factors[0] * sums[0] + factors[1] * sums[1] + factors[2] * sums[2] + factors[3] * sums[3]
    lane = lax.broadcasted_iota(jnp.int32, total.shape, 1) & (HD // 2 - 1)
    inverse = 1.0 / jnp.where(lane < heads, total, 1.0)
    weights = [f * inverse for f in factors]
    copies = []
    for t, (dst, scratch) in enumerate(((image_out, image_s), (text_out, text_s))):
        for h in range(heads):
            at = t * (HD // 2) + h
            acc = 0.0
            for key in range(SIDE):
                acc = acc + stacked(key, t * heads + h) * weights[key][:, at : at + 1]
            for g in range(SIDE):
                cols = slice(g * width + h * HD, g * width + (h + 1) * HD)
                scratch[:, cols] = acc[g * rows : (g + 1) * rows].astype(jnp.bfloat16)
        copies.append(pltpu.make_async_copy(scratch, dst, sems.at[t]))
        copies[-1].start()
    for c in copies:
        c.wait()


def local(
    image_query,
    image_key,
    image_value,
    text_query,
    text_key,
    text_value,
    image_query_gain,
    image_key_gain,
    text_query_gain,
    text_key_gain,
    image_order,
    text_length,
):
    rows, model = image_query.shape
    heads = model // HD
    width = model // SIDE
    text_rows = text_query.shape[0]
    block = text_rows // SIDE
    parts = SIDE * SIDE
    half = rows * SIDE**3 // 2
    bf, f32 = jnp.bfloat16, jnp.float32
    struct = jax.ShapeDtypeStruct
    gains = [g.reshape(1, HD) for g in (image_query_gain, image_key_gain, text_query_gain, text_key_gain)]

    own = vmem_call(
        lambda *refs: prep_kernel(heads, half, *refs),
        out_shape=[pltpu.VMEM((rows, 3 * width), bf)] * SIDE,
        in_specs=[HB] * 7,
        out_specs=[VM] * SIDE,
        scratch_shapes=[
            pltpu.SMEM((rows,), jnp.int32),
            pltpu.VMEM((1, HD), f32),
            pltpu.VMEM((rows, model), bf),
            pltpu.VMEM((rows, model), bf),
            pltpu.VMEM((rows, model), bf),
            pltpu.VMEM((1, HD), f32),
            pltpu.VMEM((1, HD), f32),
            pltpu.VMEM((rows, model), bf),
            pltpu.VMEM((rows, model), bf),
            pltpu.SemaphoreType.DMA((7,)),
        ],
        name="prep",
    )(image_order, jnp.asarray(frequencies()), image_query, image_key, image_value, gains[0], gains[1])

    from_y = [own[0]] + [exchange(own[d], HEAD_STEPS[d]) for d in range(1, SIDE)]

    qt, kt, vt, bias = vmem_call(
        text_kernel,
        out_shape=[pltpu.VMEM((block, width), bf)] * 3 + [pltpu.VMEM((8, block), f32)],
        in_specs=[HB] * 6,
        out_specs=[VM] * 4,
        scratch_shapes=[
            pltpu.SMEM((1,), jnp.int32),
            pltpu.VMEM((parts, block // parts, width), bf),
            pltpu.VMEM((block, width), bf),
            pltpu.VMEM((1, HD), f32),
            pltpu.VMEM((1, HD), f32),
            pltpu.SemaphoreType.DMA((5 + parts,)),
        ],
        cost_estimate=pl.CostEstimate(flops=20_000_000, bytes_accessed=600_000, transcendentals=0),
        name="text",
    )(text_query, text_key, text_value, gains[2], gains[3], text_length)

    kv, q = vmem_call(
        pack_kernel,
        out_shape=[pltpu.VMEM((SIDE * rows, 2 * width), bf), pltpu.VMEM((SIDE * rows, width), bf)],
        in_specs=[VM] * SIDE,
        out_specs=[VM] * 2,
        name="pack",
    )(*from_y)

    q_next = exchange(q, QUERY_STEPS[1])
    kvs = [kv]
    for i in range(1, SIDE):
        kvs.append(exchange(kv, KEY_STEPS[i]))
    q_two = vmem_call(
        join_kernel,
        out_shape=pltpu.VMEM((2 * SIDE * rows, width), bf),
        in_specs=[VM] * 2,
        out_specs=VM,
        name="join",
    )(q, q_next)
    q_last = exchange(q_two, QUERY_STEPS[2])

    partial = pl.pallas_call(
        attend_kernel,
        out_shape=pltpu.VMEM((parts, rows, 2 * width + HD), bf),
        in_specs=[VM] * 10,
        out_specs=VM,
        name="attend",
    )(*kvs, q_two, q_last, qt, kt, vt, bias)

    got = in_vmem(lax.all_to_all(partial, "seq", 0, 0, axis_index_groups=query_groups(), tiled=True))

    own_text = text_rows // SIDE**3
    return pl.pallas_call(
        combine_kernel,
        out_shape=[struct((rows, model), bf), struct((own_text, model), bf)],
        in_specs=[VM],
        out_specs=[HB] * 2,
        scratch_shapes=[
            pltpu.VMEM((rows, model), bf),
            pltpu.VMEM((own_text, model), bf),
            pltpu.SemaphoreType.DMA((2,)),
        ],
        name="combine",
    )(got)


def whole(*args):
    return tuple(local(*args))


def solution(mesh):
    token = P(("req", "seq"), None)
    text = P("req", None)
    return jax.shard_map(
        whole,
        mesh=mesh,
        in_specs=(token, token, token, text, text, text, P(), P(), P(), P(), P(("req", "seq")), P("req")),
        out_specs=(token, token),
        check_vma=False,
    )
```
